32 devices in a mesh: dp: 8 (over y, x, core), tensor: 4 (over z).
Axes of the slice: x: 2, y: 2, z: 4, core: 2. Of those that a mesh axis runs over, the one named last changes fastest.
Arguments:
- activations: bfloat16 [3072, 16384], P(('dp', 'tensor')), may hold values from -6 to 6
- out_grad: bfloat16 [3072, 16384], P('dp', 'tensor'), may hold values from -0.25 to 0.25
- block_ids: int32 [4, 12], replicated, may hold values from 0 to 127, as said below
- owner_map: int32 [8, 4], replicated, may hold values from 0 to 1, as said below
- master: float32 [1024, 16384], P('dp', 'tensor'), may hold values from -3 to 3
- moment: float32 [1024, 16384], P('dp', 'tensor'), may hold values from -3 to 3
- second: float32 [1024, 16384], P('dp', 'tensor'), may hold values from 0.01 to 2
Outputs:
- new_master: float32 [1024, 16384], P('dp', 'tensor')
- new_moment: float32 [1024, 16384], P('dp', 'tensor')
- new_second: float32 [1024, 16384], P('dp', 'tensor')
- hot_weights: bfloat16 [1024, 16384], P('dp')
- cold_recv: float32 [4096, 16384], P('dp', 'tensor')
The draws below stay inside these ranges and needn't reach their ends.
Inputs may be any that keep to these rules, and one draw needn't show every extreme that they name: `block_ids`: the 12 block numbers in a row are distinct. `owner_map`: each row has between 1 and 3 ones; some row has exactly 3 ones and some row exactly 1.
All inputs are finite; a program needn't handle non-finite values.
Results may differ from the reference program's by a relative error of at most 0.006.
Values may be sent and summed in bfloat16 or wider, within the bound.
A program may use at most 128 MiB of HBM per device.

```python
import math
import jax
import jax.numpy as jnp
from jax import lax

D = 16384
QO = 16384
BLOCK = 128
HOT = 8
COLD = 4
MOSTC = 3
TOK = 384
TOKENS = 3072
HOTR = 1024
N_DP = 8
N_TENSOR = 4


def draw_block_ids(key, part):
    keys = jax.random.split(jax.random.fold_in(key, 11), N_TENSOR)
    rows = jax.vmap(lambda single: jax.random.permutation(single, D // BLOCK)[:HOT + COLD])(keys)
    return rows.astype(jnp.int32)


def draw_owner_map(key, part):
    base = jax.random.fold_in(key, 23)
    first, second_key, third = jax.random.split(base, 3)
    counts = jax.random.randint(first, (N_DP,), COLD - MOSTC, MOSTC + 1)
    chosen = jax.random.permutation(second_key, N_DP)
    counts = counts.at[chosen[0]].set(MOSTC).at[chosen[1]].set(COLD - MOSTC)
    ranks = jax.vmap(lambda single: jax.random.permutation(single, COLD))(jax.random.split(third, N_DP))
    return (ranks < counts[:, None]).astype(jnp.int32)


def shard_levels(rng, shape, cuts, low, high):
    loudness, own = 1.0, jax.random.fold_in(rng, 6)
    for position, parts in cuts:
        draws = jnp.exp(jax.random.uniform(jax.random.fold_in(own, position), (parts,), jnp.float32, low / len(cuts), high / len(cuts)))
        loudness = loudness * jnp.repeat(draws, shape[position] // parts).reshape([-1 if axis == position else 1 for axis in range(len(shape))])
    return loudness


def bell_draw(own_key, extent, deviation, limit, shards=(), kind=jnp.bfloat16):
    factor_of = shard_levels(own_key, extent, shards, -0.22, 0.18) if shards else 1.0
    entries = jax.random.normal(own_key, extent, jnp.float32) * deviation * factor_of
    return jnp.minimum(jnp.maximum(entries, -limit), limit).astype(kind)


def setup_inputs(seed: int = 0) -> dict:
    streams_of = jax.random.split(jax.random.key(seed), 8)
    activations = bell_draw(streams_of[0], (TOKENS, D), 1.0, 6.0, ((0, 32),))
    out_grad = bell_draw(streams_of[1], (TOKENS, QO), (1.0 / TOKENS ** 0.5), 0.25, ((0, 8), (1, 4)))
    block_ids = draw_block_ids(jax.random.fold_in(streams_of[7], 71), 0)
    owner_map = draw_owner_map(jax.random.fold_in(streams_of[7], 71), 0)
    master = bell_draw(streams_of[4], (HOTR, QO), 0.5, 3.0, ((0, 8), (1, 4)), jnp.float32)
    moment = bell_draw(streams_of[5], (HOTR, QO), 0.5, 3.0, ((0, 8), (1, 4)), jnp.float32)
    second = jnp.clip(jnp.exp(math.log(2.0) - 5.2983174 * jax.random.uniform(streams_of[6], (HOTR, QO), jnp.float32) ** shard_levels(streams_of[6], (HOTR, QO), ((0, 8), (1, 4)), -0.2, 0.2)), 0.01, 2.0)
    return {"activations": activations, "out_grad": out_grad, "block_ids": block_ids, "owner_map": owner_map, "master": master, "moment": moment, "second": second}


BETA_ONE = 0.9
BETA_TWO = 0.95
ADAM_EPS = 1e-08
LEARN_RATE = 0.01
DECAY = 0.1
CORRECT_ONE = 1.0 - 0.9 ** 10
CORRECT_TWO = 1.0 - 0.95 ** 10

def pick_blocks(tok_rows, block_row):
    shaped = tok_rows.reshape(tok_rows.shape[0], D // BLOCK, BLOCK)
    return shaped[:, block_row, :].reshape(tok_rows.shape[0], block_row.shape[0] * BLOCK)

def reference(activations, out_grad, block_ids, owner_map, master, moment, second):
    qloc = QO // N_TENSOR
    hot_rows = HOT * BLOCK

    def per_index(carry, index):
        tok_rows = lax.dynamic_slice_in_dim(activations, index * TOK, TOK, 0)
        grad_rows = lax.dynamic_slice_in_dim(out_grad, index * TOK, TOK, 0)
        hot_list = []
        cold_list = []
        for group in range(N_TENSOR):
            chosen = pick_blocks(tok_rows, block_ids[group]).astype(jnp.float32)
            grad_cols = grad_rows[:, group * qloc:(group + 1) * qloc].astype(jnp.float32)
            product = jnp.dot(chosen.T, grad_cols, preferred_element_type=jnp.float32)
            hot_list.append(product[:hot_rows].astype(jnp.bfloat16).astype(jnp.float32))
            cold_list.append(product[hot_rows:].astype(jnp.bfloat16))
        return (carry + jnp.stack(hot_list), jnp.stack(cold_list))
    start_sum = jnp.zeros((N_TENSOR, hot_rows, qloc), jnp.float32)
    hot_sum, cold_parts = lax.scan(per_index, start_sum, jnp.arange(N_DP, dtype=jnp.int32))
    grad = hot_sum.transpose(1, 0, 2).reshape(hot_rows, QO)
    cold_parts = cold_parts.reshape(N_DP, N_TENSOR, COLD, BLOCK, qloc)
    from_prev = jnp.roll(cold_parts, 1, axis=0)
    from_next = jnp.roll(cold_parts, -1, axis=0)
    prev_owner = jnp.roll(owner_map, 1, axis=0)[:, None, :, None, None]
    next_owner = jnp.roll(owner_map, -1, axis=0)[:, None, :, None, None]
    total = jnp.where(prev_owner == 1, from_prev.astype(jnp.float32), 0.0)
    total = total + jnp.where(next_owner == 0, from_next.astype(jnp.float32), 0.0)
    cold_recv = total.transpose(0, 2, 3, 1, 4).reshape(N_DP * COLD * BLOCK, QO)
    new_moment = BETA_ONE * moment + (1.0 - BETA_ONE) * grad
    new_second = BETA_TWO * second + (1.0 - BETA_TWO) * grad * grad
    update = new_moment / CORRECT_ONE / (jnp.sqrt(new_second / CORRECT_TWO) + ADAM_EPS)
    new_master = master - LEARN_RATE * (update + DECAY * master)
    hot_weights = new_master.astype(jnp.bfloat16)
    return (new_master, new_moment, new_second, hot_weights, cold_recv)
```

```python
import functools

import jax
import jax.numpy as jnp
from jax import lax
from jax.experimental import pallas as pl
from jax.experimental.pallas import tpu as pltpu
from jax.sharding import PartitionSpec as P

BLOCK = 128
HOT = 8
COLD = 4
MOSTC = 3

BETA_ONE = 0.9
BETA_TWO = 0.95
ADAM_EPS = 1e-08
LEARN_RATE = 0.01
DECAY = 0.1
CORRECT_ONE = 1.0 - 0.9**10
CORRECT_TWO = 1.0 - 0.95**10

CHUNKS = 8
MESH = pl.DeviceIdType.MESH
F32 = jnp.float32
BF16 = jnp.bfloat16


def adam(grad, master, moment, second):
    new_moment = BETA_ONE * moment + (1.0 - BETA_ONE) * grad
    new_second = BETA_TWO * second + (1.0 - BETA_TWO) * grad * grad
    update = new_moment / CORRECT_ONE / (jnp.sqrt(new_second / CORRECT_TWO) + ADAM_EPS)
    return master - LEARN_RATE * (update + DECAY * master), new_moment, new_second


def halvings(n_dp):
    bits = []
    bit = n_dp // 2
    while bit >= 2:
        bits.append(bit)
        bit //= 2
    return bits


def flip(d, bit):
    return d + bit - 2 * bit * ((d // bit) % 2)


def gather_kernel(n_dp, n_t, unit, ids_ref, owner_ref, act, outbox, cold_outbox):
    i = lax.axis_index("dp")
    t = lax.axis_index("tensor")
    peer = flip(i, 1)
    bits = halvings(n_dp)
    half = outbox.shape[4] // unit

    owned = [owner_ref[i, c] for c in range(COLD)]
    ones = owned[0]
    for c in range(1, COLD):
        ones = ones + owned[c]
    place, taken, left = [], 0, ones
    for c in range(COLD):
        place.append(jnp.where(owned[c] == 1, taken, left))
        taken, left = taken + owned[c], left + 1 - owned[c]

    def column(block):
        return act[:, pl.ds(pl.multiple_of(block * BLOCK, BLOCK), BLOCK)]

    def hot_unit(group, d):
        index = (d * unit) // BLOCK
        cols = column(ids_ref[group, index])
        if unit < BLOCK:
            share = BLOCK // unit
            picked = cols[:, :unit]
            for s in range(1, share):
                picked = jnp.where(d % share == s, cols[:, s * unit : (s + 1) * unit], picked)
            cols = picked
        return cols

    for who, base in ((0, i), (1, peer)):
        for part in range(2):
            for k in range(n_t):
                group = (t + k) % n_t
                for u in range(half):
                    r = 2 * (u + half * (1 - part))
                    d = base
                    for b in bits:
                        if r & b:
                            d = flip(d, b)
                    cols = hot_unit(group, d)
                    outbox[who, part, k, :, pl.ds(u * unit, unit)] = cols
    for k in range(n_t):
        group = (t + k) % n_t
        for p in range(COLD):
            block = 0
            for c in range(COLD):
                block = block + jnp.where(place[c] == p, ids_ref[group, HOT + c], 0)
            cold_outbox[k, :, pl.ds(p * BLOCK, BLOCK)] = column(block)


def gather(n_dp, n_t, unit, ids, owner_map, activations):
    rows_tok = activations.shape[0]
    half = max(n_dp // 4, 1)
    smem = pl.BlockSpec(memory_space=pltpu.SMEM)
    vmem = pl.BlockSpec(memory_space=pltpu.VMEM)
    return pl.pallas_call(
        functools.partial(gather_kernel, n_dp, n_t, unit),
        out_shape=(
            jax.ShapeDtypeStruct((2, 2, n_t, rows_tok, half * unit), BF16),
            jax.ShapeDtypeStruct((n_t, rows_tok, COLD * BLOCK), BF16),
        ),
        in_specs=[smem, smem, vmem],
        out_specs=[vmem, vmem],
    )(ids, owner_map, activations)


def exchange_kernel(
    n_dp,
    n_t,
    outbox,
    cold_outbox,
    og_hbm,
    master_hbm,
    moment_hbm,
    second_hbm,
    grad_out,
    hot_out,
    prev_out,
    next_out,
    inbox,
    cold_inbox,
    og,
    lhs,
    cold_lhs,
    acc,
    rs_send,
    rs_recv,
    cold_send,
    master,
    moment,
    second,
    grad,
    hot_send,
    load_sem,
    sel_send_sem,
    sel_recv_sem,
    og_send_sem,
    og_recv_sem,
    rs_send_sem,
    rs_recv_sem,
    cold_send_sem,
    cold_recv_sem,
    hot_send_sem,
    hot_recv_sem,
    out_sem,
):
    i = lax.axis_index("dp")
    t = lax.axis_index("tensor")
    peer = flip(i, 1)
    rows_tok = cold_outbox.shape[1]
    tok, qlocal = og.shape[0] // 2, og.shape[1]
    units = n_dp // 2
    unit = grad.shape[0]
    half = max(units // 2, 1)
    hw = half * unit
    chunk = qlocal // CHUNKS

    loads = [
        pltpu.make_async_copy(og_hbm, og.at[pl.ds(0, tok)], load_sem.at[0]),
        pltpu.make_async_copy(master_hbm, master, load_sem.at[1]),
        pltpu.make_async_copy(moment_hbm, moment, load_sem.at[2]),
        pltpu.make_async_copy(second_hbm, second, load_sem.at[3]),
    ]
    loads[0].start()

    bits = halvings(n_dp)
    nxt, prv = (i + 1) % n_dp, (i + n_dp - 1) % n_dp
    partners = [(flip(i, b), t) for b in bits] + [(nxt, t), (prv, t), (peer, t)]
    for k in range(1, n_t):
        partners += [(i, (t + k) % n_t), (peer, (t + k) % n_t)]
    barrier = pltpu.get_barrier_semaphore()
    for partner in partners:
        pl.semaphore_signal(barrier, inc=1, device_id=partner, device_id_type=MESH)

    mine = pl.ds(t * rows_tok, rows_tok)
    for part in range(2):
        inbox[part, 0, mine, :] = outbox[0, part, 0]
    cold_inbox[mine, :] = cold_outbox[0]

    pl.semaphore_wait(barrier, len(partners))

    def sel_copy(who, part, k):
        return pltpu.make_async_remote_copy(
            src_ref=outbox.at[who, part, k],
            dst_ref=inbox.at[part, who, pl.ds(t * rows_tok, rows_tok)],
            send_sem=sel_send_sem.at[who, part, k],
            recv_sem=sel_recv_sem.at[who, part, k],
            device_id=(i if who == 0 else peer, (t + k) % n_t),
            device_id_type=MESH,
        )

    def cold_sel_copy(k):
        return pltpu.make_async_remote_copy(
            src_ref=cold_outbox.at[k],
            dst_ref=cold_inbox.at[pl.ds(t * rows_tok, rows_tok)],
            send_sem=sel_send_sem.at[0, 2, k],
            recv_sem=sel_recv_sem.at[0, 2, k],
            device_id=(i, (t + k) % n_t),
            device_id_type=MESH,
        )

    sel = {0: [], 1: [], 2: []}
    for part in range(2):
        for k in range(n_t):
            for who in range(2):
                if who or k:
                    sel[part].append(sel_copy(who, part, k))
    for k in range(1, n_t):
        sel[2].append(cold_sel_copy(k))
    og_copy = pltpu.make_async_remote_copy(
        src_ref=og_hbm,
        dst_ref=og.at[pl.ds(tok, tok)],
        send_sem=og_send_sem,
        recv_sem=og_recv_sem,
        device_id=(peer, t),
        device_id_type=MESH,
    )
    for copy in sel[0]:
        copy.start()
    og_copy.start()
    for load in loads[1:]:
        load.start()

    counts = [b // 2 for b in bits]
    offset = [sum(counts[:s]) * unit for s in range(len(bits))]

    def rs_copy(s, q):
        place_ = (pl.ds(offset[s], counts[s] * unit), pl.ds(q * chunk, chunk))
        return pltpu.make_async_remote_copy(
            src_ref=rs_send.at[place_],
            dst_ref=rs_recv.at[place_],
            send_sem=rs_send_sem.at[s, q],
            recv_sem=rs_recv_sem.at[s, q],
            device_id=(flip(i, bits[s]), t),
            device_id_type=MESH,
        )

    tile = min(512, chunk)

    def product(lhs_value_ref, rows, depth, col):
        return jnp.dot(
            lhs_value_ref[rows, :],
            og[pl.ds(0, depth), pl.ds(col, tile)],
            preferred_element_type=F32,
        )

    def wait_sel(part):
        for copy in sel[part]:
            copy.wait_recv()

    wait_sel(0)
    for part in (2, 1):
        for copy in sel[part]:
            copy.start()
    lhs[0, :, pl.ds(0, tok)] = inbox[0, 0].T
    lhs[0, :, pl.ds(tok, tok)] = inbox[0, 1].T
    loads[0].wait()
    og_copy.wait_recv()
    for q in range(CHUNKS):

        @pl.loop(0, chunk // tile)
        def _(n):
            col = pl.multiple_of(q * chunk + n * tile, tile)
            rs_send[pl.ds(0, hw), pl.ds(col, tile)] = product(
                lhs.at[0], slice(None), 2 * tok, col
            ).astype(BF16)

        rs_copy(0, q).start()

    def cold_copy(p, ahead, q):
        slot = p if ahead else p - 1
        place_ = (slot, slice(None), pl.ds(q * chunk, chunk))
        which = 0 if ahead else 1
        return pltpu.make_async_remote_copy(
            src_ref=cold_send.at[p, :, pl.ds(q * chunk, chunk)],
            dst_ref=(prev_out if ahead else next_out).at[place_],
            send_sem=cold_send_sem.at[which, slot, q],
            recv_sem=cold_recv_sem.at[which, slot, q],
            device_id=(nxt if ahead else prv, t),
            device_id_type=MESH,
        )

    wait_sel(2)
    cold_lhs[...] = cold_inbox[...].T
    for q in range(CHUNKS):

        @pl.loop(0, chunk // tile)
        def _(n):
            col = pl.multiple_of(q * chunk + n * tile, tile)
            out = product(cold_lhs, slice(None), tok, col).astype(BF16)
            for p in range(COLD):
                cold_send[p, :, pl.ds(col, tile)] = out[p * BLOCK : (p + 1) * BLOCK]

    def send_cold(q):
        for slot in range(MOSTC):
            cold_copy(slot, True, q).start()
            cold_copy(slot + COLD - MOSTC, False, q).start()

    wait_sel(1)
    lhs[1, :, pl.ds(0, tok)] = inbox[1, 0].T
    lhs[1, :, pl.ds(tok, tok)] = inbox[1, 1].T

    @pl.loop(0, qlocal // tile)
    def _(n):
        col = pl.multiple_of(n * tile, tile)
        acc[:, pl.ds(col, tile)] = product(lhs.at[1], slice(None), 2 * tok, col)

    for load in loads[1:]:
        load.wait()

    def hot_copy(up, d, q):
        origin = t - (d - 1) if up else t + (d - 1)
        cols = pl.ds(pl.multiple_of(origin * qlocal + q * chunk, chunk), chunk)
        side = 0 if up else 1
        return pltpu.make_async_remote_copy(
            src_ref=hot_send.at[:, pl.ds(q * chunk, chunk)] if d == 1 else hot_out.at[:, cols],
            dst_ref=hot_out.at[:, cols],
            send_sem=hot_send_sem.at[side, d, q],
            recv_sem=hot_recv_sem.at[side, d, q],
            device_id=(i, t + 1 if up else t - 1),
            device_id_type=MESH,
        )

    def sends(up, d):
        return (t >= d - 1) & (t < n_t - 1) if up else (t <= n_t - d) & (t > 0)

    def gets(up, d):
        return t >= d if up else t < n_t - d

    def relay(d, q):
        for up in (True, False):

            @pl.when(gets(up, d))
            def _():
                hot_copy(up, d, q).wait_recv()

            if d < n_t - 1:

                @pl.when(sends(up, d + 1))
                def _():
                    hot_copy(up, d + 1, q).start()

    def grad_store(q):
        cols = pl.ds(q * chunk, chunk)
        return pltpu.make_async_copy(grad.at[:, cols], grad_out.at[:, cols], out_sem.at[0, q])

    def hot_store(q):
        return pltpu.make_async_copy(
            hot_send.at[:, pl.ds(q * chunk, chunk)],
            hot_out.at[:, pl.ds(t * qlocal + q * chunk, chunk)],
            out_sem.at[1, q],
        )

    step = min(256, chunk)

    def settle(s, q):
        rs_copy(s, q).wait_recv()
        last = s == len(bits) - 1

        @pl.loop(0, chunk // step)
        def _(n):
            cols = pl.ds(pl.multiple_of(q * chunk + n * step, step), step)
            keep = counts[s] * unit
            got = rs_recv[pl.ds(offset[s], keep), cols].astype(F32)
            total = acc[pl.ds(0, keep), cols] + got
            if last:
                grad[:, cols] = total
                new_master, _, _ = adam(total, master[:, cols], moment[:, cols], second[:, cols])
                hot_send[:, cols] = new_master.astype(BF16)
            else:
                sent = counts[s + 1] * unit
                acc[pl.ds(0, sent), cols] = total[:sent]
                rs_send[pl.ds(offset[s + 1], sent), cols] = total[sent:].astype(BF16)

        if last:
            for up in (True, False):

                @pl.when(sends(up, 1))
                def _():
                    hot_copy(up, 1, q).start()

            grad_store(q).start()
            hot_store(q).start()
        else:
            rs_copy(s + 1, q).start()

    cold_sent = 0
    ahead = len(bits) - 1
    for wave in range(CHUNKS + ahead + n_t - 1):
        for s in reversed(range(len(bits))):
            q = wave - s
            if 0 <= q < CHUNKS:
                settle(s, q)
        for d in range(1, n_t):
            if 0 <= wave - ahead - d < CHUNKS:
                relay(d, wave - ahead - d)
        if cold_sent < CHUNKS:
            send_cold(cold_sent)
            cold_sent += 1

    for part in range(3):
        for copy in sel[part]:
            copy.wait_send()
    og_copy.wait_send()
    for q in range(CHUNKS):
        for s in range(len(bits)):
            rs_copy(s, q).wait_send()
        grad_store(q).wait()
        hot_store(q).wait()
        for d in range(1, n_t):
            for up in (True, False):

                @pl.when(sends(up, d))
                def _():
                    hot_copy(up, d, q).wait_send()

        for slot in range(MOSTC):
            cold_copy(slot, True, q).wait()
            cold_copy(slot + COLD - MOSTC, False, q).wait()


def exchange(n_dp, n_t, outbox, cold_outbox, out_grad, master, moment, second):
    tok, qlocal = out_grad.shape
    unit = master.shape[0]
    units = n_dp // 2
    half = max(units // 2, 1)
    stages = max(n_dp.bit_length() - 2, 1)
    traded = (units - 1) * unit
    vmem = pl.BlockSpec(memory_space=pltpu.VMEM)
    anywhere = pl.BlockSpec(memory_space=pl.ANY)
    dma = pltpu.SemaphoreType.DMA
    return pl.pallas_call(
        functools.partial(exchange_kernel, n_dp, n_t),
        out_shape=(
            jax.ShapeDtypeStruct((unit, qlocal), F32),
            jax.ShapeDtypeStruct((unit, qlocal * n_t), BF16),
            jax.ShapeDtypeStruct((MOSTC, BLOCK, qlocal), BF16),
            jax.ShapeDtypeStruct((MOSTC, BLOCK, qlocal), BF16),
        ),
        in_specs=[vmem, vmem] + [anywhere] * 4,
        out_specs=[anywhere] * 4,
        scratch_shapes=[
            pltpu.VMEM((2, 2, tok, half * unit), BF16),
            pltpu.VMEM((tok, COLD * BLOCK), BF16),
            pltpu.VMEM((2 * tok, qlocal), BF16),
            pltpu.VMEM((2, half * unit, 2 * tok), BF16),
            pltpu.VMEM((COLD * BLOCK, tok), BF16),
            pltpu.VMEM((half * unit, qlocal), F32),
            pltpu.VMEM((traded, qlocal), BF16),
            pltpu.VMEM((traded, qlocal), BF16),
            pltpu.VMEM((COLD, BLOCK, qlocal), BF16),
            pltpu.VMEM((unit, qlocal), F32),
            pltpu.VMEM((unit, qlocal), F32),
            pltpu.VMEM((unit, qlocal), F32),
            pltpu.VMEM((unit, qlocal), F32),
            pltpu.VMEM((unit, qlocal), BF16),
            dma((4,)),
            dma((2, 3, n_t)),
            dma((2, 3, n_t)),
            dma(()),
            dma(()),
            dma((stages, CHUNKS)),
            dma((stages, CHUNKS)),
            dma((2, MOSTC, CHUNKS)),
            dma((2, MOSTC, CHUNKS)),
            dma((2, n_t, CHUNKS)),
            dma((2, n_t, CHUNKS)),
            dma((2, CHUNKS)),
        ],
        compiler_params=pltpu.CompilerParams(
            collective_id=0, has_side_effects=True, vmem_limit_bytes=60 * 1024 * 1024
        ),
    )(outbox, cold_outbox, out_grad, master, moment, second)


def cold_kernel(where_ref, owner_ref, prev_ref, next_ref, out_ref):
    c = pl.program_id(0)
    from_prev = owner_ref[where_ref[0], c] == 1
    from_next = owner_ref[where_ref[1], c] == 0
    total = jnp.where(from_prev, prev_ref[0].astype(F32), 0.0)
    out_ref[...] = total + jnp.where(from_next, next_ref[0].astype(F32), 0.0)


def ones_before(owner_ref, row, c):
    count = 0
    for b in range(COLD):
        count = count + jnp.where(b < c, owner_ref[row, b], 0)
    return count


def prev_slot(c, n, where_ref, owner_ref):
    return jnp.minimum(ones_before(owner_ref, where_ref[0], c), MOSTC - 1), 0, n


def next_slot(c, n, where_ref, owner_ref):
    row = where_ref[1]
    ones = ones_before(owner_ref, row, COLD)
    place = ones + c - ones_before(owner_ref, row, c)
    return jnp.clip(place - (COLD - MOSTC), 0, MOSTC - 1), 0, n


def merge_cold(where, owner_map, from_prev, from_next):
    qlocal = from_prev.shape[2]
    width = qlocal
    return pl.pallas_call(
        cold_kernel,
        out_shape=jax.ShapeDtypeStruct((COLD * BLOCK, qlocal), F32),
        grid_spec=pltpu.PrefetchScalarGridSpec(
            num_scalar_prefetch=2,
            grid=(COLD, 1),
            in_specs=[
                pl.BlockSpec((1, BLOCK, width), prev_slot),
                pl.BlockSpec((1, BLOCK, width), next_slot),
            ],
            out_specs=pl.BlockSpec((BLOCK, width), lambda c, n, *_: (c, n)),
        ),
    )(where, owner_map, from_prev, from_next)


def per_device(n_dp, n_t, activations, out_grad, block_ids, owner_map, master, moment, second):
    outbox, cold_outbox = gather(n_dp, n_t, master.shape[0], block_ids, owner_map, activations)
    grad, hot_weights, from_prev, from_next = exchange(
        n_dp, n_t, outbox, cold_outbox, out_grad, master, moment, second
    )
    index = lax.axis_index("dp")
    where = jnp.stack([(index + n_dp - 1) % n_dp, (index + 1) % n_dp]).astype(jnp.int32)
    cold_recv = merge_cold(where, owner_map, from_prev, from_next)
    new_master, new_moment, new_second = adam(grad, master, moment, second)
    return (new_master, new_moment, new_second, hot_weights, cold_recv)


def solution(mesh):
    return jax.shard_map(
        functools.partial(per_device, mesh.shape["dp"], mesh.shape["tensor"]),
        mesh=mesh,
        in_specs=(
            P(("dp", "tensor"), None),
            P("dp", "tensor"),
            P(),
            P(),
            P("dp", "tensor"),
            P("dp", "tensor"),
            P("dp", "tensor"),
        ),
        out_specs=(
            P("dp", "tensor"),
            P("dp", "tensor"),
            P("dp", "tensor"),
            P("dp", None),
            P("dp", "tensor"),
        ),
        check_vma=False,
    )
```

```python
import functools

import jax
import jax.numpy as jnp
from jax import lax
from jax.experimental import pallas as pl
from jax.experimental.pallas import tpu as pltpu
from jax.sharding import PartitionSpec as P

BLOCK = 128
HOT = 8
COLD = 4
MOSTC = 3

BETA_ONE = 0.9
BETA_TWO = 0.95
ADAM_EPS = 1e-08
LEARN_RATE = 0.01
DECAY = 0.1
CORRECT_ONE = 1.0 - 0.9**10
CORRECT_TWO = 1.0 - 0.95**10

CHUNKS = 16
EARLY = 5
COLD_AT = 1
COLD_LAG = 3
MESH = pl.DeviceIdType.MESH
F32 = jnp.float32
BF16 = jnp.bfloat16


def adam(grad, master, moment, second):
    new_moment = BETA_ONE * moment + (1.0 - BETA_ONE) * grad
    new_second = BETA_TWO * second + (1.0 - BETA_TWO) * grad * grad
    update = new_moment / CORRECT_ONE / (jnp.sqrt(new_second / CORRECT_TWO) + ADAM_EPS)
    return master - LEARN_RATE * (update + DECAY * master), new_moment, new_second


def stage_bits(n_dp):
    bits = [1]
    bit = 4
    while bit < n_dp:
        bits.append(bit)
        bit *= 2
    return bits


def flip(d, bit):
    return d + bit - 2 * bit * ((d // bit) % 2)


def side_block(n_dp, unit, side, col):
    place = col // unit
    d = (place // 2) * 4 + side * 2 + place % 2
    return (d * unit + col % unit) // BLOCK


def gather_kernel(n_dp, n_t, unit, ids_ref, owner_ref, act, outbox, cold_outbox, sem):
    i = lax.axis_index("dp")
    t = lax.axis_index("tensor")
    side = (i // 2) % 2
    wide = outbox.shape[3] // BLOCK
    owned = [owner_ref[c, i] for c in range(COLD)]
    ones = owned[0]
    for c in range(1, COLD):
        ones = ones + owned[c]
    place, taken, left = [], 0, ones
    for c in range(COLD):
        place.append(jnp.where(owned[c] == 1, taken, left))
        taken, left = taken + owned[c], left + 1 - owned[c]

    copies = []

    def pull(block, target):
        cols = pl.ds(pl.multiple_of(block * BLOCK, BLOCK), BLOCK)
        copies.append(pltpu.make_async_copy(act.at[:, cols], target, sem.at[len(copies)]))
        copies[-1].start()

    for which in (1, 0):
        for k in range(n_t):
            group = (t + k) % n_t
            for b in range(wide):
                index = side_block(n_dp, unit, (side + which) % 2, b * BLOCK)
                pull(ids_ref[group, index], outbox.at[which, k, :, pl.ds(b * BLOCK, BLOCK)])
    for k in range(n_t):
        group = (t + k) % n_t
        for p in range(COLD):
            block = 0
            for c in range(COLD):
                block = block + jnp.where(place[c] == p, ids_ref[group, HOT + c], 0)
            pull(block, cold_outbox.at[k, :, pl.ds(p * BLOCK, BLOCK)])
    for copy in copies:
        copy.wait()


def gather(n_dp, n_t, unit, ids, owner_t, activations):
    rows_tok = activations.shape[0]
    wide = n_dp // 2 * unit
    smem = pl.BlockSpec(memory_space=pltpu.SMEM)
    vmem = pl.BlockSpec(memory_space=pltpu.VMEM)
    jobs = n_t * (2 * wide // BLOCK + COLD)
    return pl.pallas_call(
        functools.partial(gather_kernel, n_dp, n_t, unit),
        out_shape=(
            pltpu.VMEM((2, n_t, rows_tok, wide), BF16),
            pltpu.VMEM((n_t, rows_tok, COLD * BLOCK), BF16),
        ),
        in_specs=[smem, smem, pl.BlockSpec(memory_space=pltpu.HBM)],
        out_specs=[vmem, vmem],
        scratch_shapes=[pltpu.SemaphoreType.DMA((jobs,))],
        compiler_params=pltpu.CompilerParams(vmem_limit_bytes=61 * 1024 * 1024),
    )(ids, owner_t, activations)


def exchange_kernel(
    n_dp,
    n_t,
    owner_ref,
    outbox,
    cold_outbox,
    og_hbm,
    master_hbm,
    moment_hbm,
    second_hbm,
    master,
    moment,
    second,
    hot,
    cold,
    inbox,
    cold_inbox,
    part_inbox,
    part_cold,
    peer_cold,
    og,
    flat,
    lhs,
    cold_lhs,
    acc,
    rs_send,
    rs_recv,
    og_load_sem,
    load_sem,
    sel_send_sem,
    sel_recv_sem,
    pass_send_sem,
    pass_recv_sem,
    cold_send_sem,
    cold_recv_sem,
    peer_send_sem,
    peer_recv_sem,
    og_send_sem,
    og_recv_sem,
    rs_send_sem,
    rs_recv_sem,
    hot_send_sem,
    hot_recv_sem,
):
    i = lax.axis_index("dp")
    t = lax.axis_index("tensor")
    odd = i % 2
    peer = flip(i, 1)
    nxt, prv = (i + 1) % n_dp, (i + n_dp - 1) % n_dp
    part = (i + n_dp + 2 * odd - 1) % n_dp
    bits = stage_bits(n_dp)
    stages = len(bits)
    side_units = n_dp // 2
    unit = master.shape[1]
    wide = side_units * unit
    rows_tok = cold_outbox.shape[1]
    tok = og.shape[1] // 3
    chunk = og.shape[2]

    def cut(ref, q):
        return ref.at[:, pl.ds(pl.multiple_of(q * chunk, chunk), chunk)]

    def og_load(q):
        return pltpu.make_async_copy(
            cut(og_hbm, q), og.at[q, pl.ds(0, tok)], og_load_sem.at[q]
        )

    @pl.loop(0, CHUNKS)
    def _(q):
        og_load(q).start()

    def state_load(which, q):
        source = (master_hbm, moment_hbm, second_hbm)[which]
        target = (master, moment, second)[which]
        return pltpu.make_async_copy(cut(source, q), target.at[q], load_sem.at[which, q])

    partners = [(flip(i, b), t) for b in bits] + [(part, t)]
    partners += [(i, (t + k) % n_t) for k in range(1, n_t)]
    barrier = pltpu.get_barrier_semaphore()
    for partner in partners:
        pl.semaphore_signal(barrier, inc=1, device_id=partner, device_id_type=MESH)

    mine = pl.ds(t * rows_tok, rows_tok)

    def sel_copy(which, k):
        return pltpu.make_async_remote_copy(
            src_ref=outbox.at[which, k],
            dst_ref=inbox.at[which, mine],
            send_sem=sel_send_sem.at[which, k],
            recv_sem=sel_recv_sem.at[which, k],
            device_id=(i, (t + k) % n_t),
            device_id_type=MESH,
        )

    def cold_sel_copy(k):
        return pltpu.make_async_remote_copy(
            src_ref=cold_outbox.at[k],
            dst_ref=cold_inbox.at[mine],
            send_sem=sel_send_sem.at[2, k],
            recv_sem=sel_recv_sem.at[2, k],
            device_id=(i, (t + k) % n_t),
            device_id_type=MESH,
        )

    def pass_copy(k):
        rows = pl.ds(((t + n_t - k) % n_t) * rows_tok, rows_tok)
        return pltpu.make_async_remote_copy(
            src_ref=inbox.at[1, rows],
            dst_ref=part_inbox.at[rows],
            send_sem=pass_send_sem.at[k],
            recv_sem=pass_recv_sem.at[k],
            device_id=(part, t),
            device_id_type=MESH,
        )

    def og_copy(q):
        return pltpu.make_async_remote_copy(
            src_ref=og.at[q, pl.ds(0, tok)],
            dst_ref=og.at[q, pl.ds(tok, tok)],
            send_sem=og_send_sem.at[q],
            recv_sem=og_recv_sem.at[q],
            device_id=(part, t),
            device_id_type=MESH,
        )

    og_peer_copy = pltpu.make_async_remote_copy(
        src_ref=og.at[:, pl.ds(0, tok)],
        dst_ref=og.at[:, pl.ds(2 * tok, tok)],
        send_sem=peer_send_sem.at[0],
        recv_sem=peer_recv_sem.at[0],
        device_id=(peer, t),
        device_id_type=MESH,
    )

    inbox[1, mine] = outbox[1, 0]
    inbox[0, mine] = outbox[0, 0]
    cold_inbox[mine] = cold_outbox[0]
    pl.semaphore_wait(barrier, len(partners))
    for k in range(1, n_t):
        sel_copy(1, k).start()
    og_load(0).wait()
    og_copy(0).start()
    pass_copy(0).start()
    for k in range(1, n_t):
        sel_copy(0, k).start()
    for k in range(1, n_t):
        cold_sel_copy(k).start()

    @pl.loop(1, CHUNKS)
    def _(q):
        og_load(q).wait()

    og_peer_copy.start()

    @pl.loop(0, CHUNKS)
    def _(q):
        for which in range(3):
            state_load(which, q).start()

    for k in range(1, n_t):
        sel_copy(1, k).wait_recv()
        pass_copy(k).start()
        og_copy(k).start()
    for q in range(n_t, EARLY):
        og_copy(q).start()
    for k in range(1, n_t):
        sel_copy(0, k).wait_recv()

    def unit_at(r):
        d = i
        for index, b in enumerate(bits):
            if r & (1 << (stages - 1 - index)):
                d = flip(d, b)
        return d

    def build_hot(first, source):
        depth = pl.ds(first, tok)
        flat[:, depth] = source[...].T
        for r in range(side_units):
            d = unit_at(r)
            rows = pl.ds(pl.multiple_of(((d // 4) * 2 + d % 2) * unit, unit), unit)
            lhs[pl.ds(r * unit, unit), depth] = flat[rows, depth]

    build_hot(0, inbox.at[0])
    for k in range(n_t):
        pass_copy(k).wait_recv()
    build_hot(tok, part_inbox)

    counts = [side_units >> (s + 1) for s in range(stages)]
    offset = [sum(counts[:s]) * unit for s in range(stages)]
    early = max(EARLY, n_t)

    def rs_copy(s, q):
        place_ = (q, pl.ds(offset[s], counts[s] * unit))
        return pltpu.make_async_remote_copy(
            src_ref=rs_send.at[place_],
            dst_ref=rs_recv.at[place_],
            send_sem=rs_send_sem.at[s, q],
            recv_sem=rs_recv_sem.at[s, q],
            device_id=(flip(i, bits[s]), t),
            device_id_type=MESH,
        )

    def hot_copy(up, d, q):
        origin = t - (d - 1) if up else t + (d - 1)
        side = 0 if up else 1
        return pltpu.make_async_remote_copy(
            src_ref=hot.at[origin, q],
            dst_ref=hot.at[origin, q],
            send_sem=hot_send_sem.at[side, d, q],
            recv_sem=hot_recv_sem.at[side, d, q],
            device_id=(i, t + 1 if up else t - 1),
            device_id_type=MESH,
        )

    def sends(up, d):
        return (t >= d - 1) & (t < n_t - 1) if up else (t <= n_t - d) & (t > 0)

    def cold_pass_copy(to_part):
        first = (1 - odd) if to_part else odd
        which = 0 if to_part else 1
        return pltpu.make_async_remote_copy(
            src_ref=cold_inbox.at[:, pl.ds(pl.multiple_of(first * BLOCK, BLOCK), MOSTC * BLOCK)],
            dst_ref=part_cold if to_part else peer_cold,
            send_sem=cold_send_sem.at[which],
            recv_sem=cold_recv_sem.at[which],
            device_id=(part if to_part else peer, t),
            device_id_type=MESH,
        )

    def ones_before(row, c):
        count = 0
        for b in range(c):
            count = count + owner_ref[b, row]
        return count

    def build_cold():
        for place_, source, row, is_prev in (
            (0, part_cold, part, 1 - odd),
            (1, peer_cold, peer, odd),
        ):
            slots = [source[:, pl.ds(p * BLOCK, BLOCK)].astype(F32) for p in range(MOSTC)]
            for c in range(COLD):
                before = ones_before(row, c)
                after = ones_before(row, COLD) + c - before - (COLD - MOSTC)
                slot = before * is_prev + after * (1 - is_prev)
                taken = jnp.where(owner_ref[c, row] == is_prev, 1.0, 0.0)
                cols = jnp.zeros((tok, BLOCK), F32)
                for p in range(MOSTC):
                    cols = cols + slots[p] * (jnp.where(slot == p, 1.0, 0.0) * taken)
                cold_lhs[pl.ds(c * BLOCK, BLOCK), pl.ds(place_ * tok, tok)] = cols.astype(BF16).T

    keep = counts[0] * unit

    def products(q):
        og_copy(q).wait_recv()
        out = jnp.dot(lhs[...], og[q, pl.ds(0, 2 * tok)], preferred_element_type=F32)
        rs_send[q, pl.ds(0, keep)] = out[keep:].astype(BF16)
        rs_copy(0, q).start()
        acc[q] = out[:keep]

    def cold_products(q):
        cold[q] = jnp.dot(cold_lhs[...], og[q, pl.ds(tok, 2 * tok)], preferred_element_type=F32)

    def settle(s, q):
        rs_copy(s, q).wait_recv()
        held = counts[s] * unit
        got = rs_recv[q, pl.ds(offset[s], held)].astype(F32)
        total = acc[q, pl.ds(0, held)] + got
        if s < stages - 1:
            sent = counts[s + 1] * unit
            rs_send[q, pl.ds(offset[s + 1], sent)] = total[sent:].astype(BF16)
            rs_copy(s + 1, q).start()
            acc[q, pl.ds(0, sent)] = total[:sent]
            return
        for which in range(3):
            state_load(which, q).wait()
        new_master, new_moment, new_second = adam(total, master[q], moment[q], second[q])
        hot[t, q] = new_master.astype(BF16)
        for up in (True, False):

            @pl.when(sends(up, 1))
            def _():
                hot_copy(up, 1, q).start()

        master[q] = new_master
        moment[q] = new_moment
        second[q] = new_second

    def relay(up, d, q):
        @pl.when(sends(up, d + 1))
        def _():
            hot_copy(up, d, q).wait_recv()
            hot_copy(up, d + 1, q).start()

    def inside(q):
        return (q >= 0) & (q < CHUNKS)

    ticks = CHUNKS + max(stages + n_t - 2, COLD_LAG)

    @pl.loop(0, ticks)
    def _(tick):
        for s in reversed(range(stages)):
            q = tick - 1 - s

            @pl.when(inside(q))
            def _():
                settle(s, q)

        for d in range(1, n_t - 1):
            q = tick - stages - d

            @pl.when(inside(q))
            def _():
                relay(True, d, q)
                relay(False, d, q)

        @pl.when(tick == COLD_AT)
        def _():
            for k in range(1, n_t):
                cold_sel_copy(k).wait_recv()
            cold_pass_copy(True).start()
            cold_pass_copy(False).start()

        @pl.when(tick == COLD_LAG)
        def _():
            og_peer_copy.wait_recv()
            cold_pass_copy(True).wait_recv()
            cold_pass_copy(False).wait_recv()
            build_cold()

        @pl.when(tick + early < CHUNKS)
        def _():
            og_copy(tick + early).start()

        @pl.when(tick < CHUNKS)
        def _():
            products(tick)

        q = tick - COLD_LAG

        @pl.when(inside(q))
        def _():
            cold_products(q)

    for k in range(1, n_t):
        sel_copy(0, k).wait_send()
        sel_copy(1, k).wait_send()
        cold_sel_copy(k).wait_send()
    for k in range(n_t):
        pass_copy(k).wait_send()
    og_peer_copy.wait_send()
    cold_pass_copy(True).wait_send()
    cold_pass_copy(False).wait_send()

    @pl.loop(0, CHUNKS)
    def _(q):
        og_copy(q).wait_send()
        for s in range(stages):
            rs_copy(s, q).wait_send()
        for d in range(1, n_t):
            for up in (True, False):

                @pl.when(sends(up, d))
                def _():
                    hot_copy(up, d, q).wait_send()

                @pl.when(t == n_t - 1 if up else t == 0)
                def _():
                    hot_copy(up, d, q).wait_recv()


def exchange(n_dp, n_t, owner_t, outbox, cold_outbox, out_grad, master, moment, second):
    rows_tok = cold_outbox.shape[1]
    tok, qlocal = out_grad.shape
    unit = master.shape[0]
    chunk = qlocal // CHUNKS
    side_units = n_dp // 2
    wide = side_units * unit
    stages = len(stage_bits(n_dp))
    traded = (side_units - 1) * unit
    smem = pl.BlockSpec(memory_space=pltpu.SMEM)
    vmem = pl.BlockSpec(memory_space=pltpu.VMEM)
    hbm = pl.BlockSpec(memory_space=pltpu.HBM)
    dma = pltpu.SemaphoreType.DMA
    return pl.pallas_call(
        functools.partial(exchange_kernel, n_dp, n_t),
        out_shape=(
            pltpu.VMEM((CHUNKS, unit, chunk), F32),
            pltpu.VMEM((CHUNKS, unit, chunk), F32),
            pltpu.VMEM((CHUNKS, unit, chunk), F32),
            pltpu.VMEM((n_t, CHUNKS, unit, chunk), BF16),
            pltpu.VMEM((CHUNKS, COLD * BLOCK, chunk), F32),
        ),
        in_specs=[smem, vmem, vmem] + [hbm] * 4,
        out_specs=[vmem] * 5,
        scratch_shapes=[
            pltpu.VMEM((2, tok, wide), BF16),
            pltpu.VMEM((tok, COLD * BLOCK), BF16),
            pltpu.VMEM((tok, wide), BF16),
            pltpu.VMEM((tok, MOSTC * BLOCK), BF16),
            pltpu.VMEM((tok, MOSTC * BLOCK), BF16),
            pltpu.VMEM((CHUNKS, 3 * tok, chunk), BF16),
            pltpu.VMEM((wide, 2 * tok), BF16),
            pltpu.VMEM((wide, 2 * tok), BF16),
            pltpu.VMEM((COLD * BLOCK, 2 * tok), BF16),
            pltpu.VMEM((CHUNKS, wide // 2, chunk), F32),
            pltpu.VMEM((CHUNKS, traded, chunk), BF16),
            pltpu.VMEM((CHUNKS, traded, chunk), BF16),
            dma((CHUNKS,)),
            dma((3, CHUNKS)),
            dma((3, n_t)),
            dma((3, n_t)),
            dma((n_t,)),
            dma((n_t,)),
            dma((2,)),
            dma((2,)),
            dma((1,)),
            dma((1,)),
            dma((CHUNKS,)),
            dma((CHUNKS,)),
            dma((stages, CHUNKS)),
            dma((stages, CHUNKS)),
            dma((2, n_t, CHUNKS)),
            dma((2, n_t, CHUNKS)),
        ],
        compiler_params=pltpu.CompilerParams(
            collective_id=0, has_side_effects=True, vmem_limit_bytes=42 * 1024 * 1024
        ),
    )(owner_t, outbox, cold_outbox, out_grad, master, moment, second)


def place_kernel(n_t, master, moment, second, hot, cold, *refs):
    outs, sem = refs[:5], refs[5]
    chunk = master.shape[2]

    jobs = [(4, 0)] + [(w, 0) for w in range(3)] + [(3, g) for g in range(n_t)]

    def all_of(act):
        @pl.loop(0, CHUNKS)
        def _(q):
            for which, g in jobs:
                slot = which if which < 3 else (3 if which == 4 else 4 + g)
                source = (master, moment, second, hot.at[g], cold)[which]
                cols = pl.ds(pl.multiple_of((g * CHUNKS + q) * chunk, chunk), chunk)
                act(
                    pltpu.make_async_copy(
                        source.at[q], outs[which].at[:, cols], sem.at[slot, q]
                    )
                )

    all_of(lambda copy: copy.start())
    all_of(lambda copy: copy.wait())


def place_out(n_t, parts):
    chunks, unit, chunk = parts[0].shape
    qlocal = chunks * chunk
    vmem = pl.BlockSpec(memory_space=pltpu.VMEM)
    hbm = pl.BlockSpec(memory_space=pltpu.HBM)
    return pl.pallas_call(
        functools.partial(place_kernel, n_t),
        out_shape=(
            jax.ShapeDtypeStruct((unit, qlocal), F32),
            jax.ShapeDtypeStruct((unit, qlocal), F32),
            jax.ShapeDtypeStruct((unit, qlocal), F32),
            jax.ShapeDtypeStruct((unit, qlocal * n_t), BF16),
            jax.ShapeDtypeStruct((parts[4].shape[1], qlocal), F32),
        ),
        in_specs=[vmem] * 5,
        out_specs=[hbm] * 5,
        scratch_shapes=[pltpu.SemaphoreType.DMA((4 + n_t, CHUNKS))],
        compiler_params=pltpu.CompilerParams(vmem_limit_bytes=40 * 1024 * 1024),
    )(*parts)


def per_device(n_dp, n_t, activations, out_grad, block_ids, owner_map, master, moment, second):
    owner_t = owner_map.T
    outbox, cold_outbox = gather(n_dp, n_t, master.shape[0], block_ids, owner_t, activations)
    parts = exchange(
        n_dp, n_t, owner_t, outbox, cold_outbox, out_grad, master, moment, second
    )
    return tuple(place_out(n_t, parts))


def solution(mesh):
    return jax.shard_map(
        functools.partial(per_device, mesh.shape["dp"], mesh.shape["tensor"]),
        mesh=mesh,
        in_specs=(
            P(("dp", "tensor"), None),
            P("dp", "tensor"),
            P(),
            P(),
            P("dp", "tensor"),
            P("dp", "tensor"),
            P("dp", "tensor"),
        ),
        out_specs=(
            P("dp", "tensor"),
            P("dp", "tensor"),
            P("dp", "tensor"),
            P("dp", None),
            P("dp", "tensor"),
        ),
        check_vma=False,
    )
```

```python
import functools

import jax
import jax.numpy as jnp
from jax import lax
from jax.experimental import pallas as pl
from jax.experimental.pallas import tpu as pltpu
from jax.sharding import PartitionSpec as P

BLOCK = 128
HOT = 8
COLD = 4
MOSTC = 3

BETA_ONE = 0.9
BETA_TWO = 0.95
ADAM_EPS = 1e-08
LEARN_RATE = 0.01
DECAY = 0.1
CORRECT_ONE = 1.0 - 0.9**10
CORRECT_TWO = 1.0 - 0.95**10

CHUNKS = 16
EARLY = 4
SETTLE_LAG = 1
RELAY_LAG = 1
REACH = 2
COLD_AT = 3
COLD_LAG = CHUNKS // 2
MESH = pl.DeviceIdType.MESH
F32 = jnp.float32
BF16 = jnp.bfloat16


def adam(grad, master, moment, second):
    new_moment = BETA_ONE * moment + (1.0 - BETA_ONE) * grad
    new_second = BETA_TWO * second + (1.0 - BETA_TWO) * grad * grad
    update = new_moment / CORRECT_ONE / (jnp.sqrt(new_second / CORRECT_TWO) + ADAM_EPS)
    return master - LEARN_RATE * (update + DECAY * master), new_moment, new_second


def stage_bits(n_dp):
    bits = [1]
    bit = 4
    while bit < n_dp:
        bits.append(bit)
        bit *= 2
    return bits


def flip(d, bit):
    return d + bit - 2 * bit * ((d // bit) % 2)


def side_block(n_dp, unit, side, col):
    place = col // unit
    d = (place // 2) * 4 + side * 2 + place % 2
    return (d * unit + col % unit) // BLOCK


def gather_kernel(n_dp, n_t, unit, ids_ref, owner_ref, act, outbox, cold_outbox, sem):
    i = lax.axis_index("dp")
    t = lax.axis_index("tensor")
    side = (i // 2) % 2
    wide = outbox.shape[3] // BLOCK
    owned = [owner_ref[c, i] for c in range(COLD)]
    ones = owned[0]
    for c in range(1, COLD):
        ones = ones + owned[c]
    place, taken, left = [], 0, ones
    for c in range(COLD):
        place.append(jnp.where(owned[c] == 1, taken, left))
        taken, left = taken + owned[c], left + 1 - owned[c]

    copies = []

    def pull(block, target):
        cols = pl.ds(pl.multiple_of(block * BLOCK, BLOCK), BLOCK)
        copies.append(pltpu.make_async_copy(act.at[:, cols], target, sem.at[len(copies)]))
        copies[-1].start()

    for which in (1, 0):
        for k in range(n_t):
            group = (t + k) % n_t
            for b in range(wide):
                index = side_block(n_dp, unit, (side + which) % 2, b * BLOCK)
                pull(ids_ref[group, index], outbox.at[which, k, :, pl.ds(b * BLOCK, BLOCK)])
    for k in range(n_t):
        group = (t + k) % n_t
        for p in range(COLD):
            block = 0
            for c in range(COLD):
                block = block + jnp.where(place[c] == p, ids_ref[group, HOT + c], 0)
            pull(block, cold_outbox.at[k, :, pl.ds(p * BLOCK, BLOCK)])
    for copy in copies:
        copy.wait()


def gather(n_dp, n_t, unit, ids, owner_t, activations):
    rows_tok = activations.shape[0]
    wide = n_dp // 2 * unit
    smem = pl.BlockSpec(memory_space=pltpu.SMEM)
    vmem = pl.BlockSpec(memory_space=pltpu.VMEM)
    jobs = n_t * (2 * wide // BLOCK + COLD)
    return pl.pallas_call(
        functools.partial(gather_kernel, n_dp, n_t, unit),
        out_shape=(
            pltpu.VMEM((2, n_t, rows_tok, wide), BF16),
            pltpu.VMEM((n_t, rows_tok, COLD * BLOCK), BF16),
        ),
        in_specs=[smem, smem, pl.BlockSpec(memory_space=pltpu.HBM)],
        out_specs=[vmem, vmem],
        scratch_shapes=[pltpu.SemaphoreType.DMA((jobs,))],
        compiler_params=pltpu.CompilerParams(vmem_limit_bytes=61 * 1024 * 1024),
    )(ids, owner_t, activations)


def exchange_kernel(
    n_dp,
    n_t,
    owner_ref,
    outbox,
    cold_outbox,
    og_hbm,
    master_hbm,
    moment_hbm,
    second_hbm,
    master,
    moment,
    second,
    hot,
    cold,
    inbox,
    cold_inbox,
    part_inbox,
    part_cold,
    peer_cold,
    og,
    flat,
    lhs,
    cold_lhs,
    acc,
    rs_send,
    rs_recv,
    og_load_sem,
    load_sem,
    sel_send_sem,
    sel_recv_sem,
    pass_send_sem,
    pass_recv_sem,
    cold_send_sem,
    cold_recv_sem,
    peer_send_sem,
    peer_recv_sem,
    og_send_sem,
    og_recv_sem,
    rs_send_sem,
    rs_recv_sem,
    hot_send_sem,
    hot_recv_sem,
):
    i = lax.axis_index("dp")
    t = lax.axis_index("tensor")
    odd = i % 2
    peer = flip(i, 1)
    nxt, prv = (i + 1) % n_dp, (i + n_dp - 1) % n_dp
    part = (i + n_dp + 2 * odd - 1) % n_dp
    bits = stage_bits(n_dp)
    stages = len(bits)
    side_units = n_dp // 2
    unit = master.shape[1]
    wide = side_units * unit
    rows_tok = cold_outbox.shape[1]
    tok = og.shape[1] // 3
    chunk = og.shape[2]

    def cut(ref, q):
        return ref.at[:, pl.ds(pl.multiple_of(q * chunk, chunk), chunk)]

    def og_load(q):
        return pltpu.make_async_copy(
            cut(og_hbm, q), og.at[q, pl.ds(0, tok)], og_load_sem.at[q]
        )

    @pl.loop(0, CHUNKS)
    def _(q):
        og_load(q).start()

    def state_load(which, q):
        source = (master_hbm, moment_hbm, second_hbm)[which]
        target = (master, moment, second)[which]
        return pltpu.make_async_copy(cut(source, q), target.at[q], load_sem.at[which, q])

    partners = [(flip(i, b), t) for b in bits] + [(part, t)]
    partners += [(i, (t + k) % n_t) for k in range(1, n_t)]
    barrier = pltpu.get_barrier_semaphore()
    for partner in partners:
        pl.semaphore_signal(barrier, inc=1, device_id=partner, device_id_type=MESH)

    mine = pl.ds(t * rows_tok, rows_tok)

    def sel_copy(which, k):
        return pltpu.make_async_remote_copy(
            src_ref=outbox.at[which, k],
            dst_ref=inbox.at[which, mine],
            send_sem=sel_send_sem.at[which, k],
            recv_sem=sel_recv_sem.at[which, k],
            device_id=(i, (t + k) % n_t),
            device_id_type=MESH,
        )

    def cold_sel_copy(k):
        return pltpu.make_async_remote_copy(
            src_ref=cold_outbox.at[k],
            dst_ref=cold_inbox.at[mine],
            send_sem=sel_send_sem.at[2, k],
            recv_sem=sel_recv_sem.at[2, k],
            device_id=(i, (t + k) % n_t),
            device_id_type=MESH,
        )

    def pass_copy(k):
        rows = pl.ds(((t + n_t - k) % n_t) * rows_tok, rows_tok)
        return pltpu.make_async_remote_copy(
            src_ref=inbox.at[1, rows],
            dst_ref=part_inbox.at[rows],
            send_sem=pass_send_sem.at[k],
            recv_sem=pass_recv_sem.at[k],
            device_id=(part, t),
            device_id_type=MESH,
        )

    def og_copy(q):
        return pltpu.make_async_remote_copy(
            src_ref=og.at[q, pl.ds(0, tok)],
            dst_ref=og.at[q, pl.ds(tok, tok)],
            send_sem=og_send_sem.at[q],
            recv_sem=og_recv_sem.at[q],
            device_id=(part, t),
            device_id_type=MESH,
        )

    og_peer_copy = pltpu.make_async_remote_copy(
        src_ref=og.at[:, pl.ds(0, tok)],
        dst_ref=og.at[:, pl.ds(2 * tok, tok)],
        send_sem=peer_send_sem.at[0],
        recv_sem=peer_recv_sem.at[0],
        device_id=(peer, t),
        device_id_type=MESH,
    )

    inbox[1, mine] = outbox[1, 0]
    inbox[0, mine] = outbox[0, 0]
    cold_inbox[mine] = cold_outbox[0]
    pl.semaphore_wait(barrier, len(partners))
    lower = t < n_t // 2
    far = [jnp.where(lower, k, n_t - k) for k in range(n_t - 1, 0, -1)]
    for k in far:
        sel_copy(1, k).start()
    og_load(0).wait()
    og_copy(0).start()
    pass_copy(0).start()
    for k in far:
        sel_copy(0, k).start()
    for k in far:
        cold_sel_copy(k).start()

    @pl.loop(1, CHUNKS)
    def _(q):
        og_load(q).wait()

    og_peer_copy.start()

    @pl.loop(0, CHUNKS)
    def _(q):
        for which in range(3):
            state_load(which, q).start()

    og_copy(0).wait_recv()
    og_copy(1).start()
    for k in far:
        sel_copy(1, k).wait_recv()
        pass_copy(k).start()
    for q in range(2, EARLY):
        og_copy(q).start()
    for k in range(1, n_t):
        sel_copy(0, k).wait_recv()

    def unit_at(r):
        d = i
        for index, b in enumerate(bits):
            if r & (1 << (stages - 1 - index)):
                d = flip(d, b)
        return d

    def build_hot(first, source):
        depth = pl.ds(first, tok)
        flat[:, depth] = source[...].T
        for r in range(side_units):
            d = unit_at(r)
            rows = pl.ds(pl.multiple_of(((d // 4) * 2 + d % 2) * unit, unit), unit)
            lhs[pl.ds(r * unit, unit), depth] = flat[rows, depth]

    build_hot(0, inbox.at[0])
    for k in range(n_t):
        pass_copy(k).wait_recv()
    build_hot(tok, part_inbox)

    counts = [side_units >> (s + 1) for s in range(stages)]
    offset = [sum(counts[:s]) * unit for s in range(stages)]

    def rs_copy(s, q):
        place_ = (q, pl.ds(offset[s], counts[s] * unit))
        return pltpu.make_async_remote_copy(
            src_ref=rs_send.at[place_],
            dst_ref=rs_recv.at[place_],
            send_sem=rs_send_sem.at[s, q],
            recv_sem=rs_recv_sem.at[s, q],
            device_id=(flip(i, bits[s]), t),
            device_id_type=MESH,
        )

    def hot_copy(up, d, q):
        step = d if d <= REACH else 1
        origin = t if d <= REACH else (t - (d - 1) if up else t + (d - 1))
        side = 0 if up else 1
        return pltpu.make_async_remote_copy(
            src_ref=hot.at[origin, q],
            dst_ref=hot.at[origin, q],
            send_sem=hot_send_sem.at[side, d, q],
            recv_sem=hot_recv_sem.at[side, d, q],
            device_id=(i, t + step if up else t - step),
            device_id_type=MESH,
        )

    def gets(up, d):
        return t >= d if up else t < n_t - d

    def sends(up, d):
        if d <= REACH:
            return t < n_t - d if up else t >= d
        return (t >= d - 1) & (t < n_t - 1) if up else (t <= n_t - d) & (t > 0)

    def waits_late(up, d):
        if d < REACH:
            return gets(up, d)
        return gets(up, d) & (t == n_t - 1 if up else t == 0)

    def cold_pass_copy(to_part):
        first = (1 - odd) if to_part else odd
        which = 0 if to_part else 1
        return pltpu.make_async_remote_copy(
            src_ref=cold_inbox.at[:, pl.ds(pl.multiple_of(first * BLOCK, BLOCK), MOSTC * BLOCK)],
            dst_ref=part_cold if to_part else peer_cold,
            send_sem=cold_send_sem.at[which],
            recv_sem=cold_recv_sem.at[which],
            device_id=(part if to_part else peer, t),
            device_id_type=MESH,
        )

    def ones_before(row, c):
        count = 0
        for b in range(c):
            count = count + owner_ref[b, row]
        return count

    def build_cold():
        for place_, source, row, is_prev in (
            (0, part_cold, part, 1 - odd),
            (1, peer_cold, peer, odd),
        ):
            slots = [source[:, pl.ds(p * BLOCK, BLOCK)].astype(F32) for p in range(MOSTC)]
            for c in range(COLD):
                before = ones_before(row, c)
                after = ones_before(row, COLD) + c - before - (COLD - MOSTC)
                slot = before * is_prev + after * (1 - is_prev)
                taken = jnp.where(owner_ref[c, row] == is_prev, 1.0, 0.0)
                cols = jnp.zeros((tok, BLOCK), F32)
                for p in range(MOSTC):
                    cols = cols + slots[p] * (jnp.where(slot == p, 1.0, 0.0) * taken)
                cold_lhs[pl.ds(c * BLOCK, BLOCK), pl.ds(place_ * tok, tok)] = cols.astype(BF16).T

    keep = counts[0] * unit

    def products(q):

        @pl.when(q > 0)
        def _():
            og_copy(q).wait_recv()

        out = jnp.dot(lhs[...], og[q, pl.ds(0, 2 * tok)], preferred_element_type=F32)
        rs_send[q, pl.ds(0, keep)] = out[keep:].astype(BF16)
        rs_copy(0, q).start()
        acc[q] = out[:keep]

    def cold_products(q):
        cold[q] = jnp.dot(cold_lhs[...], og[q, pl.ds(tok, 2 * tok)], preferred_element_type=F32)

    def settle(s, q):
        rs_copy(s, q).wait_recv()
        held = counts[s] * unit
        got = rs_recv[q, pl.ds(offset[s], held)].astype(F32)
        total = acc[q, pl.ds(0, held)] + got
        if s < stages - 1:
            sent = counts[s + 1] * unit
            rs_send[q, pl.ds(offset[s + 1], sent)] = total[sent:].astype(BF16)
            rs_copy(s + 1, q).start()
            acc[q, pl.ds(0, sent)] = total[:sent]
            return
        for which in range(3):
            state_load(which, q).wait()
        new_master, new_moment, new_second = adam(total, master[q], moment[q], second[q])
        hot[t, q] = new_master.astype(BF16)
        for d in range(1, min(REACH + 1, n_t)):
            for up in (True, False):

                @pl.when(sends(up, d))
                def _():
                    hot_copy(up, d, q).start()

        master[q] = new_master
        moment[q] = new_moment
        second[q] = new_second

    def relay(up, d, q):
        @pl.when(sends(up, d + 1))
        def _():
            hot_copy(up, d, q).wait_recv()
            hot_copy(up, d + 1, q).start()

    def inside(q):
        return (q >= 0) & (q < CHUNKS)

    settled = 1 + (stages - 1) * SETTLE_LAG
    ticks = CHUNKS + settled + max(n_t - 1 - REACH, 0) * RELAY_LAG

    @pl.loop(0, ticks)
    def _(tick):
        for s in reversed(range(stages)):
            q = tick - 1 - s * SETTLE_LAG

            @pl.when(inside(q))
            def _():
                settle(s, q)

        for d in range(REACH, n_t - 1):
            q = tick - settled - (d - REACH + 1) * RELAY_LAG

            @pl.when(inside(q))
            def _():
                relay(True, d, q)
                relay(False, d, q)

        @pl.when(tick == COLD_AT)
        def _():
            for k in range(1, n_t):
                cold_sel_copy(k).wait_recv()
            cold_pass_copy(True).start()
            cold_pass_copy(False).start()

        @pl.when(tick == COLD_LAG)
        def _():
            og_peer_copy.wait_recv()
            cold_pass_copy(True).wait_recv()
            cold_pass_copy(False).wait_recv()
            build_cold()

        @pl.when(tick + EARLY < CHUNKS)
        def _():
            og_copy(tick + EARLY).start()

        @pl.when(tick < CHUNKS)
        def _():
            products(tick)

        for e in range(2):
            q = 2 * (tick - COLD_LAG) + e

            @pl.when(inside(q))
            def _():
                cold_products(q)

    for k in range(1, n_t):
        sel_copy(0, k).wait_send()
        sel_copy(1, k).wait_send()
        cold_sel_copy(k).wait_send()
    for k in range(n_t):
        pass_copy(k).wait_send()
    og_peer_copy.wait_send()
    cold_pass_copy(True).wait_send()
    cold_pass_copy(False).wait_send()

    @pl.loop(0, CHUNKS)
    def _(q):
        og_copy(q).wait_send()
        for s in range(stages):
            rs_copy(s, q).wait_send()
        for d in range(1, n_t):
            for up in (True, False):

                @pl.when(sends(up, d))
                def _():
                    hot_copy(up, d, q).wait_send()

                @pl.when(waits_late(up, d))
                def _():
                    hot_copy(up, d, q).wait_recv()


def exchange(n_dp, n_t, owner_t, outbox, cold_outbox, out_grad, master, moment, second):
    rows_tok = cold_outbox.shape[1]
    tok, qlocal = out_grad.shape
    unit = master.shape[0]
    chunk = qlocal // CHUNKS
    side_units = n_dp // 2
    wide = side_units * unit
    stages = len(stage_bits(n_dp))
    traded = (side_units - 1) * unit
    smem = pl.BlockSpec(memory_space=pltpu.SMEM)
    vmem = pl.BlockSpec(memory_space=pltpu.VMEM)
    hbm = pl.BlockSpec(memory_space=pltpu.HBM)
    dma = pltpu.SemaphoreType.DMA
    return pl.pallas_call(
        functools.partial(exchange_kernel, n_dp, n_t),
        out_shape=(
            pltpu.VMEM((CHUNKS, unit, chunk), F32),
            pltpu.VMEM((CHUNKS, unit, chunk), F32),
            pltpu.VMEM((CHUNKS, unit, chunk), F32),
            pltpu.VMEM((n_t, CHUNKS, unit, chunk), BF16),
            pltpu.VMEM((CHUNKS, COLD * BLOCK, chunk), F32),
        ),
        in_specs=[smem, vmem, vmem] + [hbm] * 4,
        out_specs=[vmem] * 5,
        scratch_shapes=[
            pltpu.VMEM((2, tok, wide), BF16),
            pltpu.VMEM((tok, COLD * BLOCK), BF16),
            pltpu.VMEM((tok, wide), BF16),
            pltpu.VMEM((tok, MOSTC * BLOCK), BF16),
            pltpu.VMEM((tok, MOSTC * BLOCK), BF16),
            pltpu.VMEM((CHUNKS, 3 * tok, chunk), BF16),
            pltpu.VMEM((wide, 2 * tok), BF16),
            pltpu.VMEM((wide, 2 * tok), BF16),
            pltpu.VMEM((COLD * BLOCK, 2 * tok), BF16),
            pltpu.VMEM((CHUNKS, wide // 2, chunk), F32),
            pltpu.VMEM((CHUNKS, traded, chunk), BF16),
            pltpu.VMEM((CHUNKS, traded, chunk), BF16),
            dma((CHUNKS,)),
            dma((3, CHUNKS)),
            dma((3, n_t)),
            dma((3, n_t)),
            dma((n_t,)),
            dma((n_t,)),
            dma((2,)),
            dma((2,)),
            dma((1,)),
            dma((1,)),
            dma((CHUNKS,)),
            dma((CHUNKS,)),
            dma((stages, CHUNKS)),
            dma((stages, CHUNKS)),
            dma((2, n_t, CHUNKS)),
            dma((2, n_t, CHUNKS)),
        ],
        compiler_params=pltpu.CompilerParams(
            collective_id=0, has_side_effects=True, vmem_limit_bytes=34 * 1024 * 1024
        ),
    )(owner_t, outbox, cold_outbox, out_grad, master, moment, second)


def place_kernel(n_t, master, moment, second, hot, cold, *refs):
    outs, sem = refs[:5], refs[5]
    chunk = master.shape[2]

    jobs = [(4, 0)] + [(w, 0) for w in range(3)] + [(3, g) for g in range(n_t)]

    def all_of(act):
        @pl.loop(0, CHUNKS)
        def _(q):
            for which, g in jobs:
                slot = which if which < 3 else (3 if which == 4 else 4 + g)
                source = (master, moment, second, hot.at[g], cold)[which]
                cols = pl.ds(pl.multiple_of((g * CHUNKS + q) * chunk, chunk), chunk)
                act(
                    pltpu.make_async_copy(
                        source.at[q], outs[which].at[:, cols], sem.at[slot, q]
                    )
                )

    all_of(lambda copy: copy.start())
    all_of(lambda copy: copy.wait())


def place_out(n_t, parts):
    chunks, unit, chunk = parts[0].shape
    qlocal = chunks * chunk
    vmem = pl.BlockSpec(memory_space=pltpu.VMEM)
    hbm = pl.BlockSpec(memory_space=pltpu.HBM)
    return pl.pallas_call(
        functools.partial(place_kernel, n_t),
        out_shape=(
            jax.ShapeDtypeStruct((unit, qlocal), F32),
            jax.ShapeDtypeStruct((unit, qlocal), F32),
            jax.ShapeDtypeStruct((unit, qlocal), F32),
            jax.ShapeDtypeStruct((unit, qlocal * n_t), BF16),
            jax.ShapeDtypeStruct((parts[4].shape[1], qlocal), F32),
        ),
        in_specs=[vmem] * 5,
        out_specs=[hbm] * 5,
        scratch_shapes=[pltpu.SemaphoreType.DMA((4 + n_t, CHUNKS))],
        compiler_params=pltpu.CompilerParams(vmem_limit_bytes=2 * 1024 * 1024),
    )(*parts)


def per_device(n_dp, n_t, activations, out_grad, block_ids, owner_map, master, moment, second):
    owner_t = owner_map.T
    outbox, cold_outbox = gather(n_dp, n_t, master.shape[0], block_ids, owner_t, activations)
    parts = exchange(
        n_dp, n_t, owner_t, outbox, cold_outbox, out_grad, master, moment, second
    )
    return tuple(place_out(n_t, parts))


def solution(mesh):
    return jax.shard_map(
        functools.partial(per_device, mesh.shape["dp"], mesh.shape["tensor"]),
        mesh=mesh,
        in_specs=(
            P(("dp", "tensor"), None),
            P("dp", "tensor"),
            P(),
            P(),
            P("dp", "tensor"),
            P("dp", "tensor"),
            P("dp", "tensor"),
        ),
        out_specs=(
            P("dp", "tensor"),
            P("dp", "tensor"),
            P("dp", "tensor"),
            P("dp", None),
            P("dp", "tensor"),
        ),
        check_vma=False,
    )
```

```python
import functools

import jax
import jax.numpy as jnp
from jax import lax
from jax.experimental import pallas as pl
from jax.experimental.pallas import tpu as pltpu
from jax.sharding import PartitionSpec as P

BLOCK = 128
HOT = 8
COLD = 4
MOSTC = 3

BETA_ONE = 0.9
BETA_TWO = 0.95
ADAM_EPS = 1e-08
LEARN_RATE = 0.01
DECAY = 0.1
CORRECT_ONE = 1.0 - 0.9**10
CORRECT_TWO = 1.0 - 0.95**10

CHUNKS = 16
FIRST = 4
EARLY = 4
MERGE_LAG = 1
SETTLE_LAG = 3
RELAY_LAG = 2
REACH = 2
COLD_STEP = 4
MESH = pl.DeviceIdType.MESH
F32 = jnp.float32
BF16 = jnp.bfloat16


def adam(grad, master, moment, second):
    new_moment = BETA_ONE * moment + (1.0 - BETA_ONE) * grad
    new_second = BETA_TWO * second + (1.0 - BETA_TWO) * grad * grad
    update = new_moment / CORRECT_ONE / (jnp.sqrt(new_second / CORRECT_TWO) + ADAM_EPS)
    return master - LEARN_RATE * (update + DECAY * master), new_moment, new_second


def phase_bit(n_dp, unit):
    return 1 if unit % BLOCK == 0 else 4


def free_bits(n_dp, unit):
    return [b for b in (1 << k for k in range(n_dp.bit_length() - 1)) if b not in (2, phase_bit(n_dp, unit))]


def flip(d, bit):
    return d + bit - 2 * bit * ((d // bit) % 2)


def phase_block(n_dp, unit, side, phase, col):
    place = col // unit
    d = side * 2 + phase * phase_bit(n_dp, unit)
    for k, b in enumerate(free_bits(n_dp, unit)):
        d = d + ((place >> k) % 2) * b
    return (d * unit + col % unit) // BLOCK


def exchange_kernel(
    n_dp,
    n_t,
    ids_ref,
    owner_ref,
    act_hbm,
    og_hbm,
    master_hbm,
    moment_hbm,
    second_hbm,
    master,
    moment,
    second,
    hot,
    cold,
    act,
    outbox,
    cold_outbox,
    inbox,
    cold_inbox,
    part_inbox,
    part_cold,
    peer_cold,
    og,
    flat,
    lhs,
    cold_lhs,
    acc,
    rs_send,
    rs_recv,
    og_load_sem,
    load_sem,
    sel_send_sem,
    sel_recv_sem,
    pass_send_sem,
    pass_recv_sem,
    cold_send_sem,
    cold_recv_sem,
    peer_send_sem,
    peer_recv_sem,
    og_send_sem,
    og_recv_sem,
    rs_send_sem,
    rs_recv_sem,
    hot_send_sem,
    hot_recv_sem,
    act_sem,
):
    i = lax.axis_index("dp")
    t = lax.axis_index("tensor")
    odd = i % 2
    peer = flip(i, 1)
    nxt, prv = (i + 1) % n_dp, (i + n_dp - 1) % n_dp
    part = (i + n_dp + 2 * odd - 1) % n_dp
    unit = master.shape[1]
    free = free_bits(n_dp, unit)
    bits = [phase_bit(n_dp, unit)] + free
    my_phase = (i // bits[0]) % 2
    stages = len(bits)
    units = n_dp // 4
    rows_tok = cold_outbox.shape[1]
    tok = og.shape[1] // 3
    chunk = og.shape[2]

    blocks = act.shape[0]

    def act_load(b):
        cols = pl.ds(pl.multiple_of(b * BLOCK, BLOCK), BLOCK)
        return pltpu.make_async_copy(act_hbm.at[:, cols], act.at[b], act_sem)

    @pl.loop(0, blocks)
    def _(b):
        act_load(b).start()

    def cut(ref, q):
        return ref.at[:, pl.ds(pl.multiple_of(q * chunk, chunk), chunk)]

    def og_load(q):
        return pltpu.make_async_copy(
            cut(og_hbm, q), og.at[q, pl.ds(0, tok)], og_load_sem.at[q]
        )

    @pl.loop(0, CHUNKS)
    def _(q):
        og_load(q).start()

    def state_load(which, q):
        source = (master_hbm, moment_hbm, second_hbm)[which]
        target = (master, moment, second)[which]
        return pltpu.make_async_copy(cut(source, q), target.at[q], load_sem.at[which, q])

    partners = [(flip(i, b), t) for b in bits] + [(part, t)]
    partners += [(i, (t + k) % n_t) for k in range(1, n_t)]
    barrier = pltpu.get_barrier_semaphore()
    for partner in partners:
        pl.semaphore_signal(barrier, inc=1, device_id=partner, device_id_type=MESH)

    owned = [owner_ref[c, i] for c in range(COLD)]
    ones = owned[0]
    for c in range(1, COLD):
        ones = ones + owned[c]
    place, taken, left = [], 0, ones
    for c in range(COLD):
        place.append(owned[c] * taken + (1 - owned[c]) * left)
        taken, left = taken + owned[c], left + 1 - owned[c]
    side = (i // 2) % 2

    def pick(phase, which):
        for k in range(n_t):
            group = (t + k) % n_t
            for b in range(outbox.shape[4] // BLOCK):
                index = phase_block(n_dp, unit, (side + which) % 2, phase, b * BLOCK)
                cols = act[ids_ref[group, index]]
                lanes = pl.ds(b * BLOCK, BLOCK)
                if k == 0:
                    inbox[which, phase, mine, lanes] = cols
                else:
                    outbox[which, phase, k, :, lanes] = cols

    def pick_cold():
        for k in range(n_t):
            group = (t + k) % n_t
            for p in range(COLD):
                block = 0
                for c in range(COLD):
                    block = block + jnp.where(place[c] == p, ids_ref[group, HOT + c], 0)
                lanes = pl.ds(p * BLOCK, BLOCK)
                if k == 0:
                    cold_inbox[mine, lanes] = act[block]
                else:
                    cold_outbox[k, :, lanes] = act[block]

    mine = pl.ds(t * rows_tok, rows_tok)

    def sel_copy(which, phase, k):
        return pltpu.make_async_remote_copy(
            src_ref=outbox.at[which, phase, k],
            dst_ref=inbox.at[which, phase, mine],
            send_sem=sel_send_sem.at[which + 2 * phase, k],
            recv_sem=sel_recv_sem.at[which + 2 * phase, k],
            device_id=(i, (t + k) % n_t),
            device_id_type=MESH,
        )

    def cold_sel_copy(k):
        return pltpu.make_async_remote_copy(
            src_ref=cold_outbox.at[k],
            dst_ref=cold_inbox.at[mine],
            send_sem=sel_send_sem.at[4, k],
            recv_sem=sel_recv_sem.at[4, k],
            device_id=(i, (t + k) % n_t),
            device_id_type=MESH,
        )

    def pass_copy(phase, k):
        rows = pl.ds(((t + n_t - k) % n_t) * rows_tok, rows_tok)
        return pltpu.make_async_remote_copy(
            src_ref=inbox.at[1, phase, rows],
            dst_ref=part_inbox.at[phase, rows],
            send_sem=pass_send_sem.at[phase, k],
            recv_sem=pass_recv_sem.at[phase, k],
            device_id=(part, t),
            device_id_type=MESH,
        )

    def og_copy(q):
        return pltpu.make_async_remote_copy(
            src_ref=og.at[q, pl.ds(0, tok)],
            dst_ref=og.at[q, pl.ds(tok, tok)],
            send_sem=og_send_sem.at[q],
            recv_sem=og_recv_sem.at[q],
            device_id=(part, t),
            device_id_type=MESH,
        )

    og_peer_copy = pltpu.make_async_remote_copy(
        src_ref=og.at[:, pl.ds(0, tok)],
        dst_ref=og.at[:, pl.ds(2 * tok, tok)],
        send_sem=peer_send_sem.at[0],
        recv_sem=peer_recv_sem.at[0],
        device_id=(peer, t),
        device_id_type=MESH,
    )

    @pl.loop(0, blocks)
    def _(b):
        act_load(b).wait()

    pick(0, 1)
    pl.semaphore_wait(barrier, len(partners))
    lower = t < n_t // 2
    far = [jnp.where(lower, k, n_t - k) for k in range(n_t - 1, 0, -1)]
    for k in far:
        sel_copy(1, 0, k).start()
    og_load(0).wait()
    og_copy(0).start()
    pass_copy(0, 0).start()
    for which, phase in ((0, 0), (1, 1), (0, 1)):
        pick(phase, which)
        for k in far:
            sel_copy(which, phase, k).start()
    pick_cold()
    for k in far:
        cold_sel_copy(k).start()

    @pl.loop(1, CHUNKS)
    def _(q):
        og_load(q).wait()

    og_peer_copy.start()

    @pl.loop(0, CHUNKS)
    def _(q):
        for which in range(3):
            state_load(which, q).start()

    og_copy(0).wait_recv()
    og_copy(1).start()
    def pass_on(phase):
        for k in far:
            sel_copy(1, phase, k).wait_recv()
            pass_copy(phase, k).start()

    pass_on(0)
    for q in range(2, EARLY):
        og_copy(q).start()

    def build_hot(phase, first, source):
        depth = pl.ds(first, tok)
        flat[:, depth] = source[...].T
        for r in range(units):
            place_ = 0
            for k, b in enumerate(free):
                bit = (i // b) % 2
                if r & (1 << (stages - 2 - k)):
                    bit = 1 - bit
                place_ = place_ + bit * (1 << k)
            rows = pl.ds(pl.multiple_of(place_ * unit, unit), unit)
            lhs[phase, pl.ds(r * unit, unit), depth] = flat[rows, depth]

    def receive_hot(phase):
        for k in far:
            sel_copy(0, phase, k).wait_recv()
        build_hot(phase, 0, inbox.at[0, phase])
        for k in range(n_t):
            pass_copy(phase, k).wait_recv()
        build_hot(phase, tok, part_inbox.at[phase])

    receive_hot(0)

    counts = [units >> s for s in range(stages)]
    offset = [sum(counts[:s]) * unit for s in range(stages)]

    def rs_copy(s, q):
        place_ = (q, pl.ds(offset[s], counts[s] * unit))
        return pltpu.make_async_remote_copy(
            src_ref=rs_send.at[place_],
            dst_ref=rs_recv.at[place_],
            send_sem=rs_send_sem.at[s, q],
            recv_sem=rs_recv_sem.at[s, q],
            device_id=(flip(i, bits[s]), t),
            device_id_type=MESH,
        )

    def hot_copy(up, d, q):
        step = d if d <= REACH else 1
        origin = t if d <= REACH else (t - (d - 1) if up else t + (d - 1))
        side = 0 if up else 1
        return pltpu.make_async_remote_copy(
            src_ref=hot.at[origin, q],
            dst_ref=hot.at[origin, q],
            send_sem=hot_send_sem.at[side, d, q],
            recv_sem=hot_recv_sem.at[side, d, q],
            device_id=(i, t + step if up else t - step),
            device_id_type=MESH,
        )

    def gets(up, d):
        return t >= d if up else t < n_t - d

    def sends(up, d):
        if d <= REACH:
            return t < n_t - d if up else t >= d
        return (t >= d - 1) & (t < n_t - 1) if up else (t <= n_t - d) & (t > 0)

    def waits_late(up, d):
        if d < REACH:
            return gets(up, d)
        return gets(up, d) & (t == n_t - 1 if up else t == 0)

    def cold_pass_copy(to_part):
        first = (1 - odd) if to_part else odd
        which = 0 if to_part else 1
        return pltpu.make_async_remote_copy(
            src_ref=cold_inbox.at[:, pl.ds(pl.multiple_of(first * BLOCK, BLOCK), MOSTC * BLOCK)],
            dst_ref=part_cold if to_part else peer_cold,
            send_sem=cold_send_sem.at[which],
            recv_sem=cold_recv_sem.at[which],
            device_id=(part if to_part else peer, t),
            device_id_type=MESH,
        )

    def ones_before(row, c):
        count = 0
        for b in range(c):
            count = count + owner_ref[b, row]
        return count

    def build_cold(place_, source, row, is_prev):
        slots = [source[:, pl.ds(p * BLOCK, BLOCK)].astype(F32) for p in range(MOSTC)]
        for c in range(COLD):
            before = ones_before(row, c)
            after = ones_before(row, COLD) + c - before - (COLD - MOSTC)
            slot = before * is_prev + after * (1 - is_prev)
            taken = jnp.where(owner_ref[c, row] == is_prev, 1.0, 0.0)
            cols = jnp.zeros((tok, BLOCK), F32)
            for p in range(MOSTC):
                cols = cols + slots[p] * (jnp.where(slot == p, 1.0, 0.0) * taken)
            cold_lhs[pl.ds(c * BLOCK, BLOCK), pl.ds(place_ * tok, tok)] = cols.astype(BF16).T

    def products(q, phase):
        @pl.when((q > 0) & (phase == 0))
        def _():
            og_copy(q).wait_recv()

        out = jnp.dot(lhs[phase], og[q, pl.ds(0, 2 * tok)], preferred_element_type=F32)

        @pl.when(my_phase == phase)
        def _():
            acc[q] = out

        @pl.when(my_phase != phase)
        def _():
            rs_send[q, pl.ds(0, units * unit)] = out.astype(BF16)
            rs_copy(0, q).start()

    def cold_products(q):
        cold[q] = jnp.dot(cold_lhs[...], og[q, pl.ds(tok, 2 * tok)], preferred_element_type=F32)

    def settle(s, q):
        rs_copy(s, q).wait_recv()
        held = counts[s] * unit
        got = rs_recv[q, pl.ds(offset[s], held)].astype(F32)
        total = acc[q, pl.ds(0, held)] + got
        if s < stages - 1:
            sent = counts[s + 1] * unit
            rs_send[q, pl.ds(offset[s + 1], sent)] = total[sent:].astype(BF16)
            rs_copy(s + 1, q).start()
            acc[q, pl.ds(0, sent)] = total[:sent]
            return
        for which in range(3):
            state_load(which, q).wait()

        new_master, new_moment, new_second = adam(total, master[q], moment[q], second[q])
        hot[t, q] = new_master.astype(BF16)
        for d in range(1, min(REACH + 1, n_t)):
            for up in (True, False):

                @pl.when(sends(up, d))
                def _():
                    hot_copy(up, d, q).start()

        master[q] = new_master
        moment[q] = new_moment
        second[q] = new_second

    def relay(up, d, q):
        @pl.when(sends(up, d + 1))
        def _():
            hot_copy(up, d, q).wait_recv()
            hot_copy(up, d + 1, q).start()

    def inside(q):
        return (q >= 0) & (q < CHUNKS)

    settled = MERGE_LAG + (stages - 1) * SETTLE_LAG
    works = 2 * CHUNKS
    cold_first = works + settled
    ticks = cold_first + max(max(n_t - 1 - REACH, 0) * RELAY_LAG, CHUNKS // COLD_STEP)

    def work(index):
        later = jnp.minimum(index // (2 * FIRST), 1)
        q = (1 - later) * (index % FIRST) + later * (index // 2)
        phase = (1 - later) * ((index // FIRST) % 2) + later * (index % 2)
        return q, phase

    def at(index, do):
        @pl.when((index >= 0) & (index < works))
        def _():
            do(*work(jnp.maximum(index, 0)))

    def owned_at(index, do):
        def when_owned(q, phase):
            @pl.when(phase == my_phase)
            def _():
                do(q)

        at(index, when_owned)

    @pl.loop(0, ticks)
    def _(tick):
        for s in reversed(range(stages)):
            owned_at(tick - MERGE_LAG - s * SETTLE_LAG, functools.partial(settle, s))

        def pass_along(d, q):
            relay(True, d, q)
            relay(False, d, q)

        for d in range(REACH, n_t - 1):
            back = settled + (d - REACH + 1) * RELAY_LAG
            owned_at(tick - back, functools.partial(pass_along, d))

        @pl.when(tick == cold_first - 1)
        def _():
            og_peer_copy.wait_recv()
            cold_pass_copy(False).wait_recv()
            build_cold(1, peer_cold, peer, odd)

        @pl.when(tick == cold_first)
        def _():
            cold_pass_copy(True).wait_recv()
            build_cold(0, part_cold, part, 1 - odd)

        @pl.when(tick == FIRST)
        def _():
            receive_hot(1)

        at(tick, products)

        @pl.when(tick == 0)
        def _():
            pass_copy(1, 0).start()
            pass_on(1)

        def feed(q, phase):
            @pl.when((phase == 0) & (q + EARLY < CHUNKS))
            def _():
                og_copy(q + EARLY).start()

            @pl.when((phase == 0) & (q + EARLY == CHUNKS - 1))
            def _():
                for k in far:
                    cold_sel_copy(k).wait_recv()
                cold_pass_copy(True).start()
                cold_pass_copy(False).start()

        at(tick, feed)

        for e in range(COLD_STEP):
            q = COLD_STEP * (tick - cold_first) + e

            @pl.when(inside(q))
            def _():
                cold_products(q)

    for k in range(1, n_t):
        for which in range(2):
            for phase in range(2):
                sel_copy(which, phase, k).wait_send()
        cold_sel_copy(k).wait_send()
    for k in range(n_t):
        pass_copy(0, k).wait_send()
        pass_copy(1, k).wait_send()
    og_peer_copy.wait_send()
    cold_pass_copy(True).wait_send()
    cold_pass_copy(False).wait_send()

    @pl.loop(0, CHUNKS)
    def _(q):
        og_copy(q).wait_send()
        for s in range(stages):
            rs_copy(s, q).wait_send()
        for d in range(1, n_t):
            for up in (True, False):

                @pl.when(sends(up, d))
                def _():
                    hot_copy(up, d, q).wait_send()

                @pl.when(waits_late(up, d))
                def _():
                    hot_copy(up, d, q).wait_recv()


def exchange(n_dp, n_t, ids, owner_t, activations, out_grad, master, moment, second):
    rows_tok, width = activations.shape
    tok, qlocal = out_grad.shape
    unit = master.shape[0]
    chunk = qlocal // CHUNKS
    units = n_dp // 4
    wide = units * unit
    stages = 1 + len(free_bits(n_dp, unit))
    traded = sum(units >> s for s in range(stages)) * unit
    smem = pl.BlockSpec(memory_space=pltpu.SMEM)
    vmem = pl.BlockSpec(memory_space=pltpu.VMEM)
    hbm = pl.BlockSpec(memory_space=pltpu.HBM)
    dma = pltpu.SemaphoreType.DMA
    return pl.pallas_call(
        functools.partial(exchange_kernel, n_dp, n_t),
        out_shape=(
            pltpu.VMEM((CHUNKS, unit, chunk), F32),
            pltpu.VMEM((CHUNKS, unit, chunk), F32),
            pltpu.VMEM((CHUNKS, unit, chunk), F32),
            pltpu.VMEM((n_t, CHUNKS, unit, chunk), BF16),
            pltpu.VMEM((CHUNKS, COLD * BLOCK, chunk), F32),
        ),
        in_specs=[smem, smem] + [hbm] * 5,
        out_specs=[vmem] * 5,
        scratch_shapes=[
            pltpu.VMEM((width // BLOCK, rows_tok, BLOCK), BF16),
            pltpu.VMEM((2, 2, n_t, rows_tok, wide), BF16),
            pltpu.VMEM((n_t, rows_tok, COLD * BLOCK), BF16),
            pltpu.VMEM((2, 2, tok, wide), BF16),
            pltpu.VMEM((tok, COLD * BLOCK), BF16),
            pltpu.VMEM((2, tok, wide), BF16),
            pltpu.VMEM((tok, MOSTC * BLOCK), BF16),
            pltpu.VMEM((tok, MOSTC * BLOCK), BF16),
            pltpu.VMEM((CHUNKS, 3 * tok, chunk), BF16),
            pltpu.VMEM((wide, 2 * tok), BF16),
            pltpu.VMEM((2, wide, 2 * tok), BF16),
            pltpu.VMEM((COLD * BLOCK, 2 * tok), BF16),
            pltpu.VMEM((CHUNKS, wide, chunk), F32),
            pltpu.VMEM((CHUNKS, traded, chunk), BF16),
            pltpu.VMEM((CHUNKS, traded, chunk), BF16),
            dma((CHUNKS,)),
            dma((3, CHUNKS)),
            dma((5, n_t)),
            dma((5, n_t)),
            dma((2, n_t)),
            dma((2, n_t)),
            dma((2,)),
            dma((2,)),
            dma((1,)),
            dma((1,)),
            dma((CHUNKS,)),
            dma((CHUNKS,)),
            dma((stages, CHUNKS)),
            dma((stages, CHUNKS)),
            dma((2, n_t, CHUNKS)),
            dma((2, n_t, CHUNKS)),
            dma(()),
        ],
        compiler_params=pltpu.CompilerParams(
            collective_id=0, has_side_effects=True, vmem_limit_bytes=40 * 1024 * 1024
        ),
    )(ids, owner_t, activations, out_grad, master, moment, second)


def place_kernel(n_t, master, moment, second, hot, cold, *refs):
    outs, sem = refs[:5], refs[5]
    chunk = master.shape[2]

    jobs = [(4, 0)] + [(w, 0) for w in range(3)] + [(3, g) for g in range(n_t)]

    def all_of(act):
        @pl.loop(0, CHUNKS)
        def _(q):
            for which, g in jobs:
                slot = which if which < 3 else (3 if which == 4 else 4 + g)
                source = (master, moment, second, hot.at[g], cold)[which]
                cols = pl.ds(pl.multiple_of((g * CHUNKS + q) * chunk, chunk), chunk)
                act(
                    pltpu.make_async_copy(
                        source.at[q], outs[which].at[:, cols], sem.at[slot, q]
                    )
                )

    all_of(lambda copy: copy.start())
    all_of(lambda copy: copy.wait())


def place_out(n_t, parts):
    chunks, unit, chunk = parts[0].shape
    qlocal = chunks * chunk
    vmem = pl.BlockSpec(memory_space=pltpu.VMEM)
    hbm = pl.BlockSpec(memory_space=pltpu.HBM)
    return pl.pallas_call(
        functools.partial(place_kernel, n_t),
        out_shape=(
            jax.ShapeDtypeStruct((unit, qlocal), F32),
            jax.ShapeDtypeStruct((unit, qlocal), F32),
            jax.ShapeDtypeStruct((unit, qlocal), F32),
            jax.ShapeDtypeStruct((unit, qlocal * n_t), BF16),
            jax.ShapeDtypeStruct((parts[4].shape[1], qlocal), F32),
        ),
        in_specs=[vmem] * 5,
        out_specs=[hbm] * 5,
        scratch_shapes=[pltpu.SemaphoreType.DMA((4 + n_t, CHUNKS))],
        compiler_params=pltpu.CompilerParams(vmem_limit_bytes=2 * 1024 * 1024),
    )(*parts)


def per_device(n_dp, n_t, activations, out_grad, block_ids, owner_map, master, moment, second):
    parts = exchange(
        n_dp, n_t, block_ids, owner_map.T, activations, out_grad, master, moment, second
    )
    return tuple(place_out(n_t, parts))


def solution(mesh):
    return jax.shard_map(
        functools.partial(per_device, mesh.shape["dp"], mesh.shape["tensor"]),
        mesh=mesh,
        in_specs=(
            P(("dp", "tensor"), None),
            P("dp", "tensor"),
            P(),
            P(),
            P("dp", "tensor"),
            P("dp", "tensor"),
            P("dp", "tensor"),
        ),
        out_specs=(
            P("dp", "tensor"),
            P("dp", "tensor"),
            P("dp", "tensor"),
            P("dp", None),
            P("dp", "tensor"),
        ),
        check_vma=False,
    )
```

```python
import functools

import jax
import jax.numpy as jnp
from jax import lax
from jax.experimental import pallas as pl
from jax.experimental.pallas import tpu as pltpu
from jax.sharding import PartitionSpec as P

BLOCK = 128
HOT = 8
COLD = 4
MOSTC = 3

BETA_ONE = 0.9
BETA_TWO = 0.95
ADAM_EPS = 1e-08
LEARN_RATE = 0.01
DECAY = 0.1
CORRECT_ONE = 1.0 - 0.9**10
CORRECT_TWO = 1.0 - 0.95**10

CHUNKS = 16
FIRST = 4
EARLY = 4
MERGE_LAG = 1
SETTLE_LAG = 3
RELAY_LAG = 2
COLD_STEP = 4
MESH = pl.DeviceIdType.MESH
F32 = jnp.float32
BF16 = jnp.bfloat16


def adam(grad, master, moment, second):
    new_moment = BETA_ONE * moment + (1.0 - BETA_ONE) * grad
    new_second = BETA_TWO * second + (1.0 - BETA_TWO) * grad * grad
    update = new_moment / CORRECT_ONE / (jnp.sqrt(new_second / CORRECT_TWO) + ADAM_EPS)
    return master - LEARN_RATE * (update + DECAY * master), new_moment, new_second


def phase_bit(n_dp, unit):
    return 1 if unit % BLOCK == 0 else 4


def free_bits(n_dp, unit):
    return [b for b in (1 << k for k in range(n_dp.bit_length() - 1)) if b not in (2, phase_bit(n_dp, unit))]


def flip(d, bit):
    return d + bit - 2 * bit * ((d // bit) % 2)


def phase_block(n_dp, unit, side, phase, col):
    place = col // unit
    d = side * 2 + phase * phase_bit(n_dp, unit)
    for k, b in enumerate(free_bits(n_dp, unit)):
        d = d + ((place >> k) % 2) * b
    return (d * unit + col % unit) // BLOCK


def exchange_kernel(
    n_dp,
    n_t,
    ids_ref,
    owner_ref,
    act_hbm,
    og_hbm,
    master_hbm,
    moment_hbm,
    second_hbm,
    master,
    moment,
    second,
    hot,
    cold,
    act,
    outbox,
    cold_outbox,
    inbox,
    cold_inbox,
    part_inbox,
    part_cold,
    peer_cold,
    og,
    flat,
    lhs,
    cold_lhs,
    acc,
    rs_send,
    rs_recv,
    og_load_sem,
    load_sem,
    sel_send_sem,
    sel_recv_sem,
    pass_send_sem,
    pass_recv_sem,
    cold_send_sem,
    cold_recv_sem,
    peer_send_sem,
    peer_recv_sem,
    og_send_sem,
    og_recv_sem,
    rs_send_sem,
    rs_recv_sem,
    hot_send_sem,
    hot_recv_sem,
    act_sem,
):
    i = lax.axis_index("dp")
    t = lax.axis_index("tensor")
    odd = i % 2
    peer = flip(i, 1)
    nxt, prv = (i + 1) % n_dp, (i + n_dp - 1) % n_dp
    part = (i + n_dp + 2 * odd - 1) % n_dp
    unit = master.shape[1]
    free = free_bits(n_dp, unit)
    bits = [phase_bit(n_dp, unit)] + free
    my_phase = (i // bits[0]) % 2
    stages = len(bits)
    units = n_dp // 4
    rows_tok = cold_outbox.shape[1]
    tok = og.shape[1] // 3
    chunk = og.shape[2]

    blocks = act.shape[0]

    def act_load(b):
        cols = pl.ds(pl.multiple_of(b * BLOCK, BLOCK), BLOCK)
        return pltpu.make_async_copy(act_hbm.at[:, cols], act.at[b], act_sem)

    @pl.loop(0, blocks)
    def _(b):
        act_load(b).start()

    def cut(ref, q):
        return ref.at[:, pl.ds(pl.multiple_of(q * chunk, chunk), chunk)]

    def og_load(q):
        return pltpu.make_async_copy(
            cut(og_hbm, q), og.at[q, pl.ds(0, tok)], og_load_sem
        )

    @pl.loop(0, CHUNKS)
    def _(q):
        og_load(q).start()

    def state_load(which, q):
        source = (master_hbm, moment_hbm, second_hbm)[which]
        target = (master, moment, second)[which]
        return pltpu.make_async_copy(cut(source, q), target.at[q], load_sem)

    partners = [(flip(i, b), t) for b in bits] + [(part, t)]
    partners += [(i, (t + k) % n_t) for k in range(1, n_t)]
    barrier = pltpu.get_barrier_semaphore()
    for partner in partners:
        pl.semaphore_signal(barrier, inc=1, device_id=partner, device_id_type=MESH)

    owned = [owner_ref[c, i] for c in range(COLD)]
    ones = owned[0]
    for c in range(1, COLD):
        ones = ones + owned[c]
    place, taken, left = [], 0, ones
    for c in range(COLD):
        place.append(owned[c] * taken + (1 - owned[c]) * left)
        taken, left = taken + owned[c], left + 1 - owned[c]
    side = (i // 2) % 2

    def pick(phase, which):
        for k in range(n_t):
            group = (t + k) % n_t
            for b in range(outbox.shape[4] // BLOCK):
                index = phase_block(n_dp, unit, (side + which) % 2, phase, b * BLOCK)
                cols = act[ids_ref[group, index]]
                lanes = pl.ds(b * BLOCK, BLOCK)
                if k == 0:
                    inbox[which, phase, mine, lanes] = cols
                else:
                    outbox[which, phase, k, :, lanes] = cols

    def pick_cold():
        for k in range(n_t):
            group = (t + k) % n_t
            for p in range(COLD):
                block = 0
                for c in range(COLD):
                    block = block + jnp.where(place[c] == p, ids_ref[group, HOT + c], 0)
                lanes = pl.ds(p * BLOCK, BLOCK)
                if k == 0:
                    cold_inbox[mine, lanes] = act[block]
                else:
                    cold_outbox[k, :, lanes] = act[block]

    mine = pl.ds(t * rows_tok, rows_tok)

    def sel_copy(which, phase, k):
        return pltpu.make_async_remote_copy(
            src_ref=outbox.at[which, phase, k],
            dst_ref=inbox.at[which, phase, mine],
            send_sem=sel_send_sem,
            recv_sem=sel_recv_sem.at[which + 2 * phase, k],
            device_id=(i, (t + k) % n_t),
            device_id_type=MESH,
        )

    def cold_sel_copy(k):
        return pltpu.make_async_remote_copy(
            src_ref=cold_outbox.at[k],
            dst_ref=cold_inbox.at[mine],
            send_sem=sel_send_sem,
            recv_sem=sel_recv_sem.at[4, k],
            device_id=(i, (t + k) % n_t),
            device_id_type=MESH,
        )

    def pass_copy(phase, k):
        rows = pl.ds(((t + n_t - k) % n_t) * rows_tok, rows_tok)
        return pltpu.make_async_remote_copy(
            src_ref=inbox.at[1, phase, rows],
            dst_ref=part_inbox.at[phase, rows],
            send_sem=pass_send_sem,
            recv_sem=pass_recv_sem.at[phase, k],
            device_id=(part, t),
            device_id_type=MESH,
        )

    def og_copy(q):
        return pltpu.make_async_remote_copy(
            src_ref=og.at[q, pl.ds(0, tok)],
            dst_ref=og.at[q, pl.ds(tok, tok)],
            send_sem=og_send_sem,
            recv_sem=og_recv_sem.at[q],
            device_id=(part, t),
            device_id_type=MESH,
        )

    og_peer_copy = pltpu.make_async_remote_copy(
        src_ref=og.at[:, pl.ds(0, tok)],
        dst_ref=og.at[:, pl.ds(2 * tok, tok)],
        send_sem=peer_send_sem.at[0],
        recv_sem=peer_recv_sem.at[0],
        device_id=(peer, t),
        device_id_type=MESH,
    )

    @pl.loop(0, blocks)
    def _(b):
        act_load(b).wait()

    pick(0, 1)
    pl.semaphore_wait(barrier, len(partners))
    lower = t < n_t // 2
    far = [jnp.where(lower, k, n_t - k) for k in range(n_t - 1, 0, -1)]
    for k in far:
        sel_copy(1, 0, k).start()
    @pl.loop(0, CHUNKS)
    def _(q):
        og_load(q).wait()

    og_copy(0).start()
    pass_copy(0, 0).start()
    og_copy(1).start()
    for which, phase in ((0, 0), (1, 1), (0, 1)):
        pick(phase, which)
        for k in far:
            sel_copy(which, phase, k).start()
    pick_cold()
    for k in far:
        cold_sel_copy(k).start()

    og_peer_copy.start()

    @pl.loop(0, CHUNKS)
    def _(q):
        for which in range(3):
            state_load(which, q).start()

    def pass_on(phase):
        for k in far:
            sel_copy(1, phase, k).wait_recv()
            pass_copy(phase, k).start()

    pass_on(0)
    for q in range(2, EARLY):
        og_copy(q).start()

    def build_hot(phase, first, source):
        depth = pl.ds(first, tok)
        flat[:, depth] = source[...].T
        for r in range(units):
            place_ = 0
            for k, b in enumerate(free):
                bit = (i // b) % 2
                if r & (1 << (stages - 2 - k)):
                    bit = 1 - bit
                place_ = place_ + bit * (1 << k)
            rows = pl.ds(pl.multiple_of(place_ * unit, unit), unit)
            lhs[phase, pl.ds(r * unit, unit), depth] = flat[rows, depth]

    def receive_hot(phase):
        for k in far:
            sel_copy(0, phase, k).wait_recv()
        build_hot(phase, 0, inbox.at[0, phase])
        for k in range(n_t):
            pass_copy(phase, k).wait_recv()
        build_hot(phase, tok, part_inbox.at[phase])

    receive_hot(0)

    @pl.loop(0, CHUNKS)
    def _(q):
        for which in range(3):
            state_load(which, q).wait()

    counts = [units >> s for s in range(stages)]
    offset = [sum(counts[:s]) * unit for s in range(stages)]

    def rs_copy(s, q):
        place_ = (q, pl.ds(offset[s], counts[s] * unit))
        return pltpu.make_async_remote_copy(
            src_ref=rs_send.at[place_],
            dst_ref=rs_recv.at[place_],
            send_sem=rs_send_sem,
            recv_sem=rs_recv_sem.at[s, q],
            device_id=(flip(i, bits[s]), t),
            device_id_type=MESH,
        )

    def hot_copy(up, d, q, direct):
        step = d if direct else 1
        back = 0 if direct else d - 1
        origin = t - back if up else t + back
        side = 0 if up else 1
        return pltpu.make_async_remote_copy(
            src_ref=hot.at[origin, q],
            dst_ref=hot.at[origin, q],
            send_sem=hot_send_sem,
            recv_sem=hot_recv_sem.at[side, d - 1, q],
            device_id=(i, t + step if up else t - step),
            device_id_type=MESH,
        )

    def gets(up, d):
        return t >= d if up else t < n_t - d

    def sends(up, d):
        if d == 1:
            return t < n_t - 1 if up else t > 0
        return t + d < n_t - 1 if up else t - d > 0

    def passes(up, d):
        if d == 1:
            return (t == n_t - 2) & (t >= 1) if up else (t == 1) & (t < n_t - 1)
        return (t >= d) & (t < n_t - 1) if up else (t < n_t - d) & (t > 0)

    def waits_late(up, d):
        late = t == n_t - 1 if up else t == 0
        if d == 1:
            late = late | ((t < n_t - 2) | (t < 1) if up else (t > 1) | (t == n_t - 1))
        return gets(up, d) & late

    def cold_pass_copy(to_part):
        first = (1 - odd) if to_part else odd
        which = 0 if to_part else 1
        return pltpu.make_async_remote_copy(
            src_ref=cold_inbox.at[:, pl.ds(pl.multiple_of(first * BLOCK, BLOCK), MOSTC * BLOCK)],
            dst_ref=part_cold if to_part else peer_cold,
            send_sem=cold_send_sem.at[which],
            recv_sem=cold_recv_sem.at[which],
            device_id=(part if to_part else peer, t),
            device_id_type=MESH,
        )

    def ones_before(row, c):
        count = 0
        for b in range(c):
            count = count + owner_ref[b, row]
        return count

    def build_cold(place_, source, row, is_prev):
        slots = [source[:, pl.ds(p * BLOCK, BLOCK)].astype(F32) for p in range(MOSTC)]
        for c in range(COLD):
            before = ones_before(row, c)
            after = ones_before(row, COLD) + c - before - (COLD - MOSTC)
            slot = before * is_prev + after * (1 - is_prev)
            taken = jnp.where(owner_ref[c, row] == is_prev, 1.0, 0.0)
            cols = jnp.zeros((tok, BLOCK), F32)
            for p in range(MOSTC):
                cols = cols + slots[p] * (jnp.where(slot == p, 1.0, 0.0) * taken)
            cold_lhs[pl.ds(c * BLOCK, BLOCK), pl.ds(place_ * tok, tok)] = cols.astype(BF16).T

    def products(q, phase):
        @pl.when(phase == 0)
        def _():
            og_copy(q).wait_recv()

        out = jnp.dot(lhs[phase], og[q, pl.ds(0, 2 * tok)], preferred_element_type=F32)

        @pl.when(my_phase == phase)
        def _():
            acc[q] = out

        @pl.when(my_phase != phase)
        def _():
            rs_send[q, pl.ds(0, units * unit)] = out.astype(BF16)
            rs_copy(0, q).start()

    def cold_products(q):
        cold[q] = jnp.dot(cold_lhs[...], og[q, pl.ds(tok, 2 * tok)], preferred_element_type=F32)

    def settle(s, q):
        rs_copy(s, q).wait_recv()
        held = counts[s] * unit
        got = rs_recv[q, pl.ds(offset[s], held)].astype(F32)
        total = acc[q, pl.ds(0, held)] + got
        if s < stages - 1:
            sent = counts[s + 1] * unit
            rs_send[q, pl.ds(offset[s + 1], sent)] = total[sent:].astype(BF16)
            rs_copy(s + 1, q).start()
            acc[q, pl.ds(0, sent)] = total[:sent]
            return
        new_master, new_moment, new_second = adam(total, master[q], moment[q], second[q])
        hot[t, q] = new_master.astype(BF16)
        for d in reversed(range(1, min(3, n_t))):
            for up in (True, False):

                @pl.when(sends(up, d))
                def _():
                    hot_copy(up, d, q, True).start()

        master[q] = new_master
        moment[q] = new_moment
        second[q] = new_second

    def relay(up, d, q):
        @pl.when(passes(up, d))
        def _():
            hot_copy(up, d, q, True).wait_recv()
            hot_copy(up, d + 1, q, False).start()

    def inside(q):
        return (q >= 0) & (q < CHUNKS)

    settled = MERGE_LAG + (stages - 1) * SETTLE_LAG
    works = 2 * CHUNKS
    cold_first = works + settled
    ticks = cold_first + max((n_t - 2) * RELAY_LAG, CHUNKS // COLD_STEP)

    def work(index):
        later = jnp.minimum(index // (2 * FIRST), 1)
        q = (1 - later) * (index % FIRST) + later * (index // 2)
        phase = (1 - later) * ((index // FIRST) % 2) + later * (index % 2)
        return q, phase

    def at(index, do):
        @pl.when((index >= 0) & (index < works))
        def _():
            do(*work(jnp.maximum(index, 0)))

    def owned_at(index, do):
        def when_owned(q, phase):
            @pl.when(phase == my_phase)
            def _():
                do(q)

        at(index, when_owned)

    @pl.loop(0, ticks)
    def _(tick):
        for s in reversed(range(stages)):
            owned_at(tick - MERGE_LAG - s * SETTLE_LAG, functools.partial(settle, s))

        def pass_along(d, q):
            relay(True, d, q)
            relay(False, d, q)

        for d in range(1, n_t - 1):
            back = settled + max(d - 1, 1) * RELAY_LAG
            owned_at(tick - back, functools.partial(pass_along, d))

        @pl.when(tick == cold_first - 1)
        def _():
            og_peer_copy.wait_recv()
            cold_pass_copy(False).wait_recv()
            build_cold(1, peer_cold, peer, odd)

        @pl.when(tick == cold_first)
        def _():
            cold_pass_copy(True).wait_recv()
            build_cold(0, part_cold, part, 1 - odd)

        @pl.when(tick == FIRST)
        def _():
            receive_hot(1)

        at(tick, products)

        @pl.when(tick == 0)
        def _():
            pass_copy(1, 0).start()
            pass_on(1)

        def feed(q, phase):
            @pl.when((phase == 0) & (q + EARLY < CHUNKS))
            def _():
                og_copy(q + EARLY).start()

            @pl.when((phase == 0) & (q + EARLY == CHUNKS - 1))
            def _():
                for k in far:
                    cold_sel_copy(k).wait_recv()
                cold_pass_copy(True).start()
                cold_pass_copy(False).start()

        at(tick, feed)

        for e in range(COLD_STEP):
            q = COLD_STEP * (tick - cold_first) + e

            @pl.when(inside(q))
            def _():
                cold_products(q)

    for k in range(1, n_t):
        for which in range(2):
            for phase in range(2):
                sel_copy(which, phase, k).wait_send()
        cold_sel_copy(k).wait_send()
    for k in range(n_t):
        pass_copy(0, k).wait_send()
        pass_copy(1, k).wait_send()
    og_peer_copy.wait_send()
    cold_pass_copy(True).wait_send()
    cold_pass_copy(False).wait_send()

    @pl.loop(0, CHUNKS)
    def _(q):
        og_copy(q).wait_send()
        for s in range(stages):
            rs_copy(s, q).wait_send()
        for d in range(1, n_t):
            for up in (True, False):

                sent = passes(up, d - 1) if d > 1 else t < 0
                sent = sent | sends(up, d) if d < 3 else sent

                @pl.when(sent)
                def _():
                    hot_copy(up, d, q, True).wait_send()

                @pl.when(waits_late(up, d))
                def _():
                    hot_copy(up, d, q, True).wait_recv()


def exchange(n_dp, n_t, ids, owner_t, activations, out_grad, master, moment, second):
    rows_tok, width = activations.shape
    tok, qlocal = out_grad.shape
    unit = master.shape[0]
    chunk = qlocal // CHUNKS
    units = n_dp // 4
    wide = units * unit
    stages = 1 + len(free_bits(n_dp, unit))
    traded = sum(units >> s for s in range(stages)) * unit
    smem = pl.BlockSpec(memory_space=pltpu.SMEM)
    vmem = pl.BlockSpec(memory_space=pltpu.VMEM)
    hbm = pl.BlockSpec(memory_space=pltpu.HBM)
    dma = pltpu.SemaphoreType.DMA
    return pl.pallas_call(
        functools.partial(exchange_kernel, n_dp, n_t),
        out_shape=(
            pltpu.VMEM((CHUNKS, unit, chunk), F32),
            pltpu.VMEM((CHUNKS, unit, chunk), F32),
            pltpu.VMEM((CHUNKS, unit, chunk), F32),
            pltpu.VMEM((n_t, CHUNKS, unit, chunk), BF16),
            pltpu.VMEM((CHUNKS, COLD * BLOCK, chunk), F32),
        ),
        in_specs=[smem, smem] + [hbm] * 5,
        out_specs=[vmem] * 5,
        scratch_shapes=[
            pltpu.VMEM((width // BLOCK, rows_tok, BLOCK), BF16),
            pltpu.VMEM((2, 2, n_t, rows_tok, wide), BF16),
            pltpu.VMEM((n_t, rows_tok, COLD * BLOCK), BF16),
            pltpu.VMEM((2, 2, tok, wide), BF16),
            pltpu.VMEM((tok, COLD * BLOCK), BF16),
            pltpu.VMEM((2, tok, wide), BF16),
            pltpu.VMEM((tok, MOSTC * BLOCK), BF16),
            pltpu.VMEM((tok, MOSTC * BLOCK), BF16),
            pltpu.VMEM((CHUNKS, 3 * tok, chunk), BF16),
            pltpu.VMEM((wide, 2 * tok), BF16),
            pltpu.VMEM((2, wide, 2 * tok), BF16),
            pltpu.VMEM((COLD * BLOCK, 2 * tok), BF16),
            pltpu.VMEM((CHUNKS, wide, chunk), F32),
            pltpu.VMEM((CHUNKS, traded, chunk), BF16),
            pltpu.VMEM((CHUNKS, traded, chunk), BF16),
            dma(()),
            dma(()),
            dma(()),
            dma((5, n_t)),
            dma(()),
            dma((2, n_t)),
            dma((2,)),
            dma((2,)),
            dma((1,)),
            dma((1,)),
            dma(()),
            dma((CHUNKS,)),
            dma(()),
            dma((stages, CHUNKS)),
            dma(()),
            dma((2, n_t - 1, CHUNKS)),
            dma(()),
        ],
        compiler_params=pltpu.CompilerParams(
            collective_id=0, has_side_effects=True, vmem_limit_bytes=40 * 1024 * 1024
        ),
    )(ids, owner_t, activations, out_grad, master, moment, second)


def place_kernel(n_t, master, moment, second, hot, cold, *refs):
    outs, sem = refs[:5], refs[5]
    chunk = master.shape[2]

    jobs = [(4, 0)] + [(w, 0) for w in range(3)] + [(3, g) for g in range(n_t)]

    def all_of(act):
        @pl.loop(0, CHUNKS)
        def _(q):
            for which, g in jobs:
                source = (master, moment, second, hot.at[g], cold)[which]
                cols = pl.ds(pl.multiple_of((g * CHUNKS + q) * chunk, chunk), chunk)
                act(pltpu.make_async_copy(source.at[q], outs[which].at[:, cols], sem))

    all_of(lambda copy: copy.start())
    all_of(lambda copy: copy.wait())


def place_out(n_t, parts):
    chunks, unit, chunk = parts[0].shape
    qlocal = chunks * chunk
    vmem = pl.BlockSpec(memory_space=pltpu.VMEM)
    hbm = pl.BlockSpec(memory_space=pltpu.HBM)
    return pl.pallas_call(
        functools.partial(place_kernel, n_t),
        out_shape=(
            jax.ShapeDtypeStruct((unit, qlocal), F32),
            jax.ShapeDtypeStruct((unit, qlocal), F32),
            jax.ShapeDtypeStruct((unit, qlocal), F32),
            jax.ShapeDtypeStruct((unit, qlocal * n_t), BF16),
            jax.ShapeDtypeStruct((parts[4].shape[1], qlocal), F32),
        ),
        in_specs=[vmem] * 5,
        out_specs=[hbm] * 5,
        scratch_shapes=[pltpu.SemaphoreType.DMA],
        compiler_params=pltpu.CompilerParams(vmem_limit_bytes=2 * 1024 * 1024),
    )(*parts)


def per_device(n_dp, n_t, activations, out_grad, block_ids, owner_map, master, moment, second):
    parts = exchange(
        n_dp, n_t, block_ids, owner_map.T, activations, out_grad, master, moment, second
    )
    return tuple(place_out(n_t, parts))


def solution(mesh):
    return jax.shard_map(
        functools.partial(per_device, mesh.shape["dp"], mesh.shape["tensor"]),
        mesh=mesh,
        in_specs=(
            P(("dp", "tensor"), None),
            P("dp", "tensor"),
            P(),
            P(),
            P("dp", "tensor"),
            P("dp", "tensor"),
            P("dp", "tensor"),
        ),
        out_specs=(
            P("dp", "tensor"),
            P("dp", "tensor"),
            P("dp", "tensor"),
            P("dp", None),
            P("dp", "tensor"),
        ),
        check_vma=False,
    )
```

```python
import functools

import jax
import jax.numpy as jnp
from jax import lax
from jax.experimental import pallas as pl
from jax.experimental.pallas import tpu as pltpu
from jax.sharding import PartitionSpec as P

BLOCK = 128
HOT = 8
COLD = 4
MOSTC = 3

BETA_ONE = 0.9
BETA_TWO = 0.95
ADAM_EPS = 1e-08
LEARN_RATE = 0.01
DECAY = 0.1
CORRECT_ONE = 1.0 - 0.9**10
CORRECT_TWO = 1.0 - 0.95**10

CHUNKS = 16
STRIDE = 8
FIRST = 4
EARLY = 4
MERGE_LAG = 1
SETTLE_LAG = 3
RELAY_LAG = 2
COLD_STEP = 4
MESH = pl.DeviceIdType.MESH
F32 = jnp.float32
BF16 = jnp.bfloat16


def adam(grad, master, moment, second):
    new_moment = BETA_ONE * moment + (1.0 - BETA_ONE) * grad
    new_second = BETA_TWO * second + (1.0 - BETA_TWO) * grad * grad
    update = new_moment / CORRECT_ONE / (jnp.sqrt(new_second / CORRECT_TWO) + ADAM_EPS)
    return master - LEARN_RATE * (update + DECAY * master), new_moment, new_second


def phase_bit(n_dp, unit):
    return 1 if unit % BLOCK == 0 else 4


def free_bits(n_dp, unit):
    return [b for b in (1 << k for k in range(n_dp.bit_length() - 1)) if b not in (2, phase_bit(n_dp, unit))]


def flip(d, bit):
    return d + bit - 2 * bit * ((d // bit) % 2)


def phase_block(n_dp, unit, side, phase, col):
    place = col // unit
    d = side * 2 + phase * phase_bit(n_dp, unit)
    for k, b in enumerate(free_bits(n_dp, unit)):
        d = d + ((place >> k) % 2) * b
    return (d * unit + col % unit) // BLOCK


def exchange_kernel(
    n_dp,
    n_t,
    ids_ref,
    owner_ref,
    act_hbm,
    og_hbm,
    master_hbm,
    moment_hbm,
    second_hbm,
    master,
    moment,
    second,
    hot,
    cold,
    act,
    outbox,
    cold_outbox,
    inbox,
    cold_inbox,
    part_inbox,
    part_cold,
    peer_cold,
    og,
    flat,
    lhs,
    cold_lhs,
    acc,
    rs_send,
    rs_recv,
    og_load_sem,
    load_sem,
    sel_send_sem,
    sel_recv_sem,
    pass_send_sem,
    pass_recv_sem,
    cold_send_sem,
    cold_recv_sem,
    peer_send_sem,
    peer_recv_sem,
    og_send_sem,
    og_recv_sem,
    rs_send_sem,
    rs_recv_sem,
    hot_send_sem,
    hot_recv_sem,
    act_sem,
):
    i = lax.axis_index("dp")
    t = lax.axis_index("tensor")
    odd = i % 2
    peer = flip(i, 1)
    nxt, prv = (i + 1) % n_dp, (i + n_dp - 1) % n_dp
    part = (i + n_dp + 2 * odd - 1) % n_dp
    unit = master.shape[1]
    free = free_bits(n_dp, unit)
    bits = [phase_bit(n_dp, unit)] + free
    my_phase = (i // bits[0]) % 2
    stages = len(bits)
    units = n_dp // 4
    rows_tok = cold_outbox.shape[1]
    tok = og.shape[1] // 3
    chunk = og.shape[2]

    partners = [(flip(i, b), t) for b in bits] + [(part, t)]
    partners += [(i, (t + k) % n_t) for k in range(1, n_t)]
    barrier = pltpu.get_barrier_semaphore()
    for partner in partners:
        pl.semaphore_signal(barrier, inc=1, device_id=partner, device_id_type=MESH)

    blocks = act.shape[0]

    def act_load(b):
        cols = pl.ds(pl.multiple_of(b * BLOCK, BLOCK), BLOCK)
        return pltpu.make_async_copy(act_hbm.at[:, cols], act.at[b], act_sem)

    @pl.loop(0, blocks // STRIDE)
    def _(b):
        for e in range(STRIDE):
            act_load(b * STRIDE + e).start()

    def cut(ref, q):
        return ref.at[:, pl.ds(pl.multiple_of(q * chunk, chunk), chunk)]

    def og_load(q):
        return pltpu.make_async_copy(
            cut(og_hbm, q), og.at[q, pl.ds(0, tok)], og_load_sem
        )

    @pl.loop(0, CHUNKS)
    def _(q):
        og_load(q).start()

    def state_load(which, q):
        source = (master_hbm, moment_hbm, second_hbm)[which]
        target = (master, moment, second)[which]
        return pltpu.make_async_copy(cut(source, q), target.at[q], load_sem)

    owned = [owner_ref[c, i] for c in range(COLD)]
    ones = owned[0]
    for c in range(1, COLD):
        ones = ones + owned[c]
    place, taken, left = [], 0, ones
    for c in range(COLD):
        place.append(owned[c] * taken + (1 - owned[c]) * left)
        taken, left = taken + owned[c], left + 1 - owned[c]
    side = (i // 2) % 2

    def pick(phase, which):
        for k in range(n_t):
            group = (t + k) % n_t
            for b in range(outbox.shape[4] // BLOCK):
                index = phase_block(n_dp, unit, (side + which) % 2, phase, b * BLOCK)
                cols = act[ids_ref[group, index]]
                lanes = pl.ds(b * BLOCK, BLOCK)
                if k == 0:
                    inbox[which, phase, mine, lanes] = cols
                else:
                    outbox[which, phase, k, :, lanes] = cols

    def pick_cold():
        for k in range(n_t):
            group = (t + k) % n_t
            for p in range(COLD):
                block = 0
                for c in range(COLD):
                    block = block + jnp.where(place[c] == p, ids_ref[group, HOT + c], 0)
                lanes = pl.ds(p * BLOCK, BLOCK)
                if k == 0:
                    cold_inbox[mine, lanes] = act[block]
                else:
                    cold_outbox[k, :, lanes] = act[block]

    mine = pl.ds(t * rows_tok, rows_tok)

    def sel_copy(which, phase, k):
        return pltpu.make_async_remote_copy(
            src_ref=outbox.at[which, phase, k],
            dst_ref=inbox.at[which, phase, mine],
            send_sem=sel_send_sem,
            recv_sem=sel_recv_sem.at[which + 2 * phase, k],
            device_id=(i, (t + k) % n_t),
            device_id_type=MESH,
        )

    def cold_sel_copy(k):
        return pltpu.make_async_remote_copy(
            src_ref=cold_outbox.at[k],
            dst_ref=cold_inbox.at[mine],
            send_sem=sel_send_sem,
            recv_sem=sel_recv_sem.at[4, k],
            device_id=(i, (t + k) % n_t),
            device_id_type=MESH,
        )

    def pass_copy(phase, k):
        rows = pl.ds(((t + n_t - k) % n_t) * rows_tok, rows_tok)
        return pltpu.make_async_remote_copy(
            src_ref=inbox.at[1, phase, rows],
            dst_ref=part_inbox.at[phase, rows],
            send_sem=pass_send_sem,
            recv_sem=pass_recv_sem.at[phase, k],
            device_id=(part, t),
            device_id_type=MESH,
        )

    def og_copy(q):
        return pltpu.make_async_remote_copy(
            src_ref=og.at[q, pl.ds(0, tok)],
            dst_ref=og.at[q, pl.ds(tok, tok)],
            send_sem=og_send_sem,
            recv_sem=og_recv_sem.at[q],
            device_id=(part, t),
            device_id_type=MESH,
        )

    og_peer_copy = pltpu.make_async_remote_copy(
        src_ref=og.at[:, pl.ds(0, tok)],
        dst_ref=og.at[:, pl.ds(2 * tok, tok)],
        send_sem=peer_send_sem.at[0],
        recv_sem=peer_recv_sem.at[0],
        device_id=(peer, t),
        device_id_type=MESH,
    )

    @pl.loop(0, blocks // STRIDE)
    def _(b):
        for e in range(STRIDE):
            act_load(b * STRIDE + e).wait()

    pick(0, 1)
    pl.semaphore_wait(barrier, len(partners))
    lower = t < n_t // 2
    far = [jnp.where(lower, k, n_t - k) for k in range(n_t - 1, 0, -1)]
    for k in far:
        sel_copy(1, 0, k).start()

    @pl.loop(0, CHUNKS)
    def _(q):
        og_load(q).wait()

    og_copy(0).start()
    pass_copy(0, 0).start()
    og_copy(1).start()
    for which, phase in ((0, 0), (1, 1), (0, 1)):
        pick(phase, which)
        for k in far:
            sel_copy(which, phase, k).start()
    pick_cold()
    for k in far:
        cold_sel_copy(k).start()

    og_peer_copy.start()

    @pl.loop(0, CHUNKS)
    def _(q):
        for which in range(3):
            state_load(which, q).start()

    def pass_on(phase):
        for k in far:
            sel_copy(1, phase, k).wait_recv()
            pass_copy(phase, k).start()

    pass_on(0)
    for q in range(2, EARLY):
        og_copy(q).start()

    def build_hot(phase, first, source):
        depth = pl.ds(first, tok)
        flat[:, depth] = source[...].T
        for r in range(units):
            place_ = 0
            for k, b in enumerate(free):
                bit = (i // b) % 2
                if r & (1 << (stages - 2 - k)):
                    bit = 1 - bit
                place_ = place_ + bit * (1 << k)
            rows = pl.ds(pl.multiple_of(place_ * unit, unit), unit)
            lhs[phase, pl.ds(r * unit, unit), depth] = flat[rows, depth]

    def receive_hot(phase):
        for k in far:
            sel_copy(0, phase, k).wait_recv()
        build_hot(phase, 0, inbox.at[0, phase])
        for k in range(n_t):
            pass_copy(phase, k).wait_recv()
        build_hot(phase, tok, part_inbox.at[phase])

    receive_hot(0)

    counts = [units >> s for s in range(stages)]
    offset = [sum(counts[:s]) * unit for s in range(stages)]

    def rs_copy(s, q):
        place_ = (q, pl.ds(offset[s], counts[s] * unit))
        return pltpu.make_async_remote_copy(
            src_ref=rs_send.at[place_],
            dst_ref=rs_recv.at[place_],
            send_sem=rs_send_sem,
            recv_sem=rs_recv_sem.at[s, q],
            device_id=(flip(i, bits[s]), t),
            device_id_type=MESH,
        )

    def hot_copy(up, d, q, direct):
        step = d if direct else 1
        back = 0 if direct else d - 1
        origin = t - back if up else t + back
        return pltpu.make_async_remote_copy(
            src_ref=hot.at[origin, q],
            dst_ref=hot.at[origin, q],
            send_sem=hot_send_sem,
            recv_sem=hot_recv_sem.at[origin, q],
            device_id=(i, t + step if up else t - step),
            device_id_type=MESH,
        )

    def arrival(up, d, q):
        origin = t - d if up else t + d
        return pltpu.make_async_remote_copy(
            src_ref=hot.at[origin, q],
            dst_ref=hot.at[origin, q],
            send_sem=hot_send_sem,
            recv_sem=hot_recv_sem.at[origin, q],
            device_id=(i, origin),
            device_id_type=MESH,
        )

    def gets(up, d):
        return t >= d if up else t < n_t - d

    def sends(up, d):
        if d == 1:
            return t < n_t - 1 if up else t > 0
        return t + d < n_t - 1 if up else t - d > 0

    def passes(up, d):
        if d == 1:
            return (t == n_t - 2) & (t >= 1) if up else (t == 1) & (t < n_t - 1)
        return (t >= d) & (t < n_t - 1) if up else (t < n_t - d) & (t > 0)

    def waits_late(up, d):
        late = t == n_t - 1 if up else t == 0
        if d == 1:
            late = late | ((t < n_t - 2) | (t < 1) if up else (t > 1) | (t == n_t - 1))
        return gets(up, d) & late

    def cold_pass_copy(to_part):
        first = (1 - odd) if to_part else odd
        which = 0 if to_part else 1
        return pltpu.make_async_remote_copy(
            src_ref=cold_inbox.at[:, pl.ds(pl.multiple_of(first * BLOCK, BLOCK), MOSTC * BLOCK)],
            dst_ref=part_cold if to_part else peer_cold,
            send_sem=cold_send_sem.at[which],
            recv_sem=cold_recv_sem.at[which],
            device_id=(part if to_part else peer, t),
            device_id_type=MESH,
        )

    def ones_before(row, c):
        count = 0
        for b in range(c):
            count = count + owner_ref[b, row]
        return count

    def build_cold(place_, source, row, is_prev):
        slots = [source[:, pl.ds(p * BLOCK, BLOCK)].astype(F32) for p in range(MOSTC)]
        for c in range(COLD):
            before = ones_before(row, c)
            after = ones_before(row, COLD) + c - before - (COLD - MOSTC)
            slot = before * is_prev + after * (1 - is_prev)
            taken = jnp.where(owner_ref[c, row] == is_prev, 1.0, 0.0)
            cols = jnp.zeros((tok, BLOCK), F32)
            for p in range(MOSTC):
                cols = cols + slots[p] * (jnp.where(slot == p, 1.0, 0.0) * taken)
            cold_lhs[pl.ds(c * BLOCK, BLOCK), pl.ds(place_ * tok, tok)] = cols.astype(BF16).T

    def products(q, phase):
        @pl.when(phase == 0)
        def _():
            og_copy(q).wait_recv()

        out = jnp.dot(lhs[phase], og[q, pl.ds(0, 2 * tok)], preferred_element_type=F32)

        @pl.when(my_phase == phase)
        def _():
            acc[q] = out

        @pl.when(my_phase != phase)
        def _():
            rs_send[q, pl.ds(0, units * unit)] = out.astype(BF16)
            rs_copy(0, q).start()

    def cold_products(q):
        cold[q] = jnp.dot(cold_lhs[...], og[q, pl.ds(tok, 2 * tok)], preferred_element_type=F32)

    def settle(s, q):
        rs_copy(s, q).wait_recv()
        held = counts[s] * unit
        got = rs_recv[q, pl.ds(offset[s], held)].astype(F32)
        total = acc[q, pl.ds(0, held)] + got
        if s < stages - 1:
            sent = counts[s + 1] * unit
            rs_send[q, pl.ds(offset[s + 1], sent)] = total[sent:].astype(BF16)
            rs_copy(s + 1, q).start()
            acc[q, pl.ds(0, sent)] = total[:sent]
            return
        new_master, new_moment, new_second = adam(total, master[q], moment[q], second[q])
        hot[t, q] = new_master.astype(BF16)
        for d in reversed(range(1, min(3, n_t))):
            for up in (True, False):

                @pl.when(sends(up, d))
                def _():
                    hot_copy(up, d, q, True).start()

        master[q] = new_master
        moment[q] = new_moment
        second[q] = new_second

    def relay(up, d, q):
        @pl.when(passes(up, d))
        def _():
            arrival(up, d, q).wait_recv()
            hot_copy(up, d + 1, q, False).start()

    def inside(q):
        return (q >= 0) & (q < CHUNKS)

    settled = MERGE_LAG + (stages - 1) * SETTLE_LAG
    works = 2 * CHUNKS
    cold_first = works + settled
    ticks = cold_first + max((n_t - 2) * RELAY_LAG, CHUNKS // COLD_STEP)

    def work(index):
        later = jnp.minimum(index // (2 * FIRST), 1)
        q = (1 - later) * (index % FIRST) + later * (index // 2)
        phase = (1 - later) * ((index // FIRST) % 2) + later * (index % 2)
        return q, phase

    def at(index, do):
        @pl.when((index >= 0) & (index < works))
        def _():
            do(*work(jnp.maximum(index, 0)))

    def owned_at(index, do):
        def when_owned(q, phase):
            @pl.when(phase == my_phase)
            def _():
                do(q)

        at(index, when_owned)

    @pl.loop(0, ticks)
    def _(tick):
        for s in reversed(range(stages)):
            owned_at(tick - MERGE_LAG - s * SETTLE_LAG, functools.partial(settle, s))

        def pass_along(d, q):
            relay(True, d, q)
            relay(False, d, q)

        for d in range(1, n_t - 1):
            back = settled + max(d - 1, 1) * RELAY_LAG
            owned_at(tick - back, functools.partial(pass_along, d))

        @pl.when(tick == cold_first - 1)
        def _():
            og_peer_copy.wait_recv()
            cold_pass_copy(False).wait_recv()
            build_cold(1, peer_cold, peer, odd)

        @pl.when(tick == cold_first)
        def _():
            cold_pass_copy(True).wait_recv()
            build_cold(0, part_cold, part, 1 - odd)

        @pl.when(tick == FIRST)
        def _():
            receive_hot(1)

        @pl.when(tick == 1)
        def _():
            @pl.loop(0, CHUNKS)
            def _(q):
                for which in range(3):
                    state_load(which, q).wait()

        at(tick, products)

        @pl.when(tick == 0)
        def _():
            pass_copy(1, 0).start()
            pass_on(1)

        def feed(q, phase):
            @pl.when((phase == 0) & (q + EARLY < CHUNKS))
            def _():
                og_copy(q + EARLY).start()

            @pl.when((phase == 0) & (q + EARLY == CHUNKS - 1))
            def _():
                for k in far:
                    cold_sel_copy(k).wait_recv()
                cold_pass_copy(True).start()
                cold_pass_copy(False).start()

        at(tick, feed)

        for e in range(COLD_STEP):
            q = COLD_STEP * (tick - cold_first) + e

            @pl.when(inside(q))
            def _():
                cold_products(q)

    for k in range(1, n_t):
        for which in range(2):
            for phase in range(2):
                sel_copy(which, phase, k).wait_send()
        cold_sel_copy(k).wait_send()
    for k in range(n_t):
        pass_copy(0, k).wait_send()
        pass_copy(1, k).wait_send()
    og_peer_copy.wait_send()
    cold_pass_copy(True).wait_send()
    cold_pass_copy(False).wait_send()

    @pl.loop(0, CHUNKS)
    def _(q):
        og_copy(q).wait_send()
        for s in range(stages):
            rs_copy(s, q).wait_send()
        for d in range(1, n_t):
            for up in (True, False):

                sent = passes(up, d - 1) if d > 1 else t < 0
                sent = sent | sends(up, d) if d < 3 else sent

                @pl.when(sent)
                def _():
                    hot_copy(up, d, q, True).wait_send()

                @pl.when(waits_late(up, d))
                def _():
                    arrival(up, d, q).wait_recv()


def exchange(n_dp, n_t, ids, owner_t, activations, out_grad, master, moment, second):
    rows_tok, width = activations.shape
    tok, qlocal = out_grad.shape
    unit = master.shape[0]
    chunk = qlocal // CHUNKS
    units = n_dp // 4
    wide = units * unit
    stages = 1 + len(free_bits(n_dp, unit))
    traded = sum(units >> s for s in range(stages)) * unit
    smem = pl.BlockSpec(memory_space=pltpu.SMEM)
    vmem = pl.BlockSpec(memory_space=pltpu.VMEM)
    hbm = pl.BlockSpec(memory_space=pltpu.HBM)
    dma = pltpu.SemaphoreType.DMA
    return pl.pallas_call(
        functools.partial(exchange_kernel, n_dp, n_t),
        out_shape=(
            pltpu.VMEM((CHUNKS, unit, chunk), F32),
            pltpu.VMEM((CHUNKS, unit, chunk), F32),
            pltpu.VMEM((CHUNKS, unit, chunk), F32),
            pltpu.VMEM((n_t, CHUNKS, unit, chunk), BF16),
            pltpu.VMEM((CHUNKS, COLD * BLOCK, chunk), F32),
        ),
        in_specs=[smem, smem] + [hbm] * 5,
        out_specs=[vmem] * 5,
        scratch_shapes=[
            pltpu.VMEM((width // BLOCK, rows_tok, BLOCK), BF16),
            pltpu.VMEM((2, 2, n_t, rows_tok, wide), BF16),
            pltpu.VMEM((n_t, rows_tok, COLD * BLOCK), BF16),
            pltpu.VMEM((2, 2, tok, wide), BF16),
            pltpu.VMEM((tok, COLD * BLOCK), BF16),
            pltpu.VMEM((2, tok, wide), BF16),
            pltpu.VMEM((tok, MOSTC * BLOCK), BF16),
            pltpu.VMEM((tok, MOSTC * BLOCK), BF16),
            pltpu.VMEM((CHUNKS, 3 * tok, chunk), BF16),
            pltpu.VMEM((wide, 2 * tok), BF16),
            pltpu.VMEM((2, wide, 2 * tok), BF16),
            pltpu.VMEM((COLD * BLOCK, 2 * tok), BF16),
            pltpu.VMEM((CHUNKS, wide, chunk), F32),
            pltpu.VMEM((CHUNKS, traded, chunk), BF16),
            pltpu.VMEM((CHUNKS, traded, chunk), BF16),
            dma(()),
            dma(()),
            dma(()),
            dma((5, n_t)),
            dma(()),
            dma((2, n_t)),
            dma((2,)),
            dma((2,)),
            dma((1,)),
            dma((1,)),
            dma(()),
            dma((CHUNKS,)),
            dma(()),
            dma((stages, CHUNKS)),
            dma(()),
            dma((n_t, CHUNKS)),
            dma(()),
        ],
        compiler_params=pltpu.CompilerParams(
            collective_id=0, has_side_effects=True, vmem_limit_bytes=40 * 1024 * 1024
        ),
    )(ids, owner_t, activations, out_grad, master, moment, second)


def place_kernel(n_t, master, moment, second, hot, cold, *refs):
    outs, sem = refs[:5], refs[5]
    chunk = master.shape[2]

    jobs = [(4, 0)] + [(w, 0) for w in range(3)] + [(3, g) for g in range(n_t)]

    def all_of(act):
        @pl.loop(0, CHUNKS)
        def _(q):
            for which, g in jobs:
                source = (master, moment, second, hot.at[g], cold)[which]
                cols = pl.ds(pl.multiple_of((g * CHUNKS + q) * chunk, chunk), chunk)
                act(pltpu.make_async_copy(source.at[q], outs[which].at[:, cols], sem))

    all_of(lambda copy: copy.start())
    all_of(lambda copy: copy.wait())


def place_out(n_t, parts):
    chunks, unit, chunk = parts[0].shape
    qlocal = chunks * chunk
    vmem = pl.BlockSpec(memory_space=pltpu.VMEM)
    hbm = pl.BlockSpec(memory_space=pltpu.HBM)
    return pl.pallas_call(
        functools.partial(place_kernel, n_t),
        out_shape=(
            jax.ShapeDtypeStruct((unit, qlocal), F32),
            jax.ShapeDtypeStruct((unit, qlocal), F32),
            jax.ShapeDtypeStruct((unit, qlocal), F32),
            jax.ShapeDtypeStruct((unit, qlocal * n_t), BF16),
            jax.ShapeDtypeStruct((parts[4].shape[1], qlocal), F32),
        ),
        in_specs=[vmem] * 5,
        out_specs=[hbm] * 5,
        scratch_shapes=[pltpu.SemaphoreType.DMA],
        compiler_params=pltpu.CompilerParams(vmem_limit_bytes=2 * 1024 * 1024),
    )(*parts)


def per_device(n_dp, n_t, activations, out_grad, block_ids, owner_map, master, moment, second):
    parts = exchange(
        n_dp, n_t, block_ids, owner_map.T, activations, out_grad, master, moment, second
    )
    return tuple(place_out(n_t, parts))


def solution(mesh):
    return jax.shard_map(
        functools.partial(per_device, mesh.shape["dp"], mesh.shape["tensor"]),
        mesh=mesh,
        in_specs=(
            P(("dp", "tensor"), None),
            P("dp", "tensor"),
            P(),
            P(),
            P("dp", "tensor"),
            P("dp", "tensor"),
            P("dp", "tensor"),
        ),
        out_specs=(
            P("dp", "tensor"),
            P("dp", "tensor"),
            P("dp", "tensor"),
            P("dp", None),
            P("dp", "tensor"),
        ),
        check_vma=False,
    )
```
